32 devices in a mesh: morton: 16 (over z, y, x), dp: 2 (over core).
Axes of the slice: x: 2, y: 2, z: 4, core: 2. Of those that a mesh axis runs over, the one named last changes fastest.
Arguments:
- node_feat: bfloat16 [2, 8192, 128], P('dp', 'morton'), may hold values from -6 to 6
- edge_feat: bfloat16 [2, 32768, 128], P('dp', 'morton'), may hold values from -6 to 6
- cot_node: bfloat16 [2, 8192, 128], P('dp', 'morton'), may hold values from -6 to 6
- cot_edge: bfloat16 [2, 32768, 128], P('dp', 'morton'), may hold values from -6 to 6
- senders: int32 [2, 32768], P('dp', 'morton'), may hold values from 0 to 767, as said below
- receivers: int32 [2, 32768], P('dp', 'morton'), may hold values from 0 to 511
- send_rows: int32 [2, 4096], P('dp', 'morton'), may hold values from 0 to 511
- edge_count: int32 [2, 16], P('dp', 'morton'), may hold values from 512 to 2048, as said below
- edge_w1: float32 [384, 128], replicated, may hold values from -0.3125 to 0.3125
- edge_w2: float32 [128, 128], replicated, may hold values from -0.5 to 0.5
- edge_gain: float32 [128], replicated, may hold values from 0.25 to 1.75
- node_w1: float32 [256, 128], replicated, may hold values from -0.375 to 0.375
- node_w2: float32 [128, 128], replicated, may hold values from -0.5 to 0.5
- node_gain: float32 [128], replicated, may hold values from 0.25 to 1.75
Outputs:
- grad_node: float32 [2, 8192, 128], P('dp', 'morton')
- grad_edge: float32 [2, 32768, 128], P('dp', 'morton')
- grad_edge_w1: float32 [384, 128], replicated
- grad_edge_w2: float32 [128, 128], replicated
- grad_edge_gain: float32 [128], replicated
- grad_node_w1: float32 [256, 128], replicated
- grad_node_w2: float32 [128, 128], replicated
- grad_node_gain: float32 [128], replicated
The draws below stay inside these ranges and needn't reach their ends.
Inputs may be any that keep to these rules, and one draw needn't show every extreme that they name: `senders`: on device m, an entry below 512 is one of its own cells; an entry 512 + k * 64 + q is ghost row q of group k, which comes from device m - d_k with d = (-16/2, -1, +1, +16/2); that device always exists. `send_rows`: entry k * 64 + q of device m is its local cell sent to device m + d_k, with d = (-16/2, -1, +1, +16/2). `edge_count`: edge slots at or beyond the count are empty; some device of every block is full.
All inputs are finite; a program needn't handle non-finite values.
Results may differ from the reference program's by a relative error of at most 0.014.
Values may be sent and summed in bfloat16 or wider, within the bound.
No kernel may reach another device: no remote copies, remote signals or barrier semaphores. Data moves between devices by JAX's collectives and lax.ppermute only.
A program may use at most 64 MiB of HBM per device.

```python
import jax
import jax.numpy as jnp
from jax import lax

H = 128
C_DEV = 512
GQ = 64
E_DEV = 2048
BLOCKS = 2
CELLS = 8192
EDGES = 32768
N_MORTON = 16


def draw_senders(key, part):
    raw = jax.random.randint(key, (BLOCKS, EDGES), 0, C_DEV + 4 * GQ)
    device = (jnp.arange(EDGES) // E_DEV)[None, :]
    group = jnp.clip((raw - C_DEV) // GQ, 0, 3)
    offset = jnp.array([-(N_MORTON // 2), -1, 1, N_MORTON // 2], jnp.int32)[group]
    owner = device - offset
    wrong = (raw >= C_DEV) & ((owner < 0) | (owner >= N_MORTON))
    return jnp.where(wrong, raw % C_DEV, raw).astype(jnp.int32)


def draw_edge_count(key, part):
    counts = jax.random.randint(key, (BLOCKS, N_MORTON), E_DEV // 4, E_DEV + 1)
    fuller = jax.random.randint(jax.random.fold_in(key, 7), (BLOCKS,), 0, N_MORTON)
    chosen = jnp.arange(N_MORTON)[None, :] == fuller[:, None]
    return jnp.where(chosen, E_DEV, counts).astype(jnp.int32)


def touch_ends(values, key, low, top_value):
    shape = values.shape
    spot = [jax.random.randint(jax.random.fold_in(key, axis), (), 0, shape[axis]) for axis in range(len(shape))]
    values = values.at[tuple(spot)].set(low)
    longest = shape.index(max(shape))
    spot[longest] = (spot[longest] + 1) % shape[longest]
    return values.at[tuple(spot)].set(top_value)


def level_of(own_key, shape, split, low, largest):
    level = 1.0
    for position, blocks in split:
        steps = jax.random.uniform(jax.random.fold_in(jax.random.fold_in(own_key, 6), position), (blocks,), jnp.float32, low / len(split), largest / len(split))
        level = level * jnp.repeat(jnp.exp(steps), shape[position] // blocks).reshape((-1,) + (1,) * (len(shape) - 1 - position))
    return level


def scatter_about(key, extent, scale, reach, pieces=(), kind=jnp.bfloat16):
    values = scale * jax.random.normal(key, extent, jnp.float32)
    if pieces:
        values = values * level_of(key, extent, pieces, -0.22, 0.18)
    return jnp.clip(values, -reach, reach).astype(kind)


def setup_inputs(seed: int = 0) -> dict:
    keys = jax.random.split(jax.random.key(seed), 15)
    node_feat = scatter_about(keys[0], (BLOCKS, CELLS, H), 1.0, 6.0, ((0, 2), (1, 16)))
    edge_feat = scatter_about(keys[1], (BLOCKS, EDGES, H), 1.0, 6.0, ((0, 2), (1, 16)))
    cot_node = scatter_about(keys[2], (BLOCKS, CELLS, H), 1.0, 6.0, ((0, 2), (1, 16)))
    cot_edge = scatter_about(keys[3], (BLOCKS, EDGES, H), 1.0, 6.0, ((0, 2), (1, 16)))
    senders = draw_senders(jax.random.fold_in(keys[14], 71), 0)
    receivers = touch_ends(jax.random.randint(keys[5], (BLOCKS, EDGES), 0, C_DEV), jax.random.fold_in(keys[5], 1), 0, C_DEV - 1).astype(jnp.int32)
    send_rows = touch_ends(jax.random.randint(keys[6], (BLOCKS, N_MORTON * 4 * GQ), 0, C_DEV), jax.random.fold_in(keys[6], 1), 0, C_DEV - 1).astype(jnp.int32)
    edge_count = draw_edge_count(jax.random.fold_in(keys[14], 71), 0)
    edge_w1 = scatter_about(keys[8], (3 * H, H), (3 * H) ** -0.5, 0.3125, (), jnp.float32)
    edge_w2 = scatter_about(keys[9], (H, H), H ** -0.5, 0.5, (), jnp.float32)
    edge_gain = jnp.clip(1.0 + 0.15 * jax.random.normal(keys[10], (H,), jnp.float32), 0.25, 1.75)
    node_w1 = scatter_about(keys[11], (2 * H, H), (2 * H) ** -0.5, 0.375, (), jnp.float32)
    node_w2 = scatter_about(keys[12], (H, H), H ** -0.5, 0.5, (), jnp.float32)
    node_gain = jnp.clip(1.0 + 0.15 * jax.random.normal(keys[13], (H,), jnp.float32), 0.25, 1.75)
    return {"node_feat": node_feat, "edge_feat": edge_feat, "cot_node": cot_node, "cot_edge": cot_edge, "senders": senders, "receivers": receivers, "send_rows": send_rows, "edge_count": edge_count, "edge_w1": edge_w1, "edge_w2": edge_w2, "edge_gain": edge_gain, "node_w1": node_w1, "node_w2": node_w2, "node_gain": node_gain}


def layer_norm(values, gain):
    center = values - lax.optimization_barrier(jnp.mean(values, axis=-1, keepdims=True))
    spread = lax.optimization_barrier(jnp.mean(center * center, axis=-1, keepdims=True))
    return center * lax.rsqrt(spread + 1e-05) * gain

def local_forward(cells, ghosts, edges, ew1, ew2, egain, nw1, nw2, ngain, sending, receiving, count):
    table = jnp.concatenate([cells, ghosts], axis=0)
    joined = jnp.concatenate([edges.astype(jnp.bfloat16), table[sending].astype(jnp.bfloat16), cells[receiving].astype(jnp.bfloat16)], axis=1)
    first = jnp.dot(joined, ew1.astype(jnp.bfloat16), preferred_element_type=jnp.float32)
    second = jnp.dot(jax.nn.silu(first).astype(jnp.bfloat16), ew2.astype(jnp.bfloat16), preferred_element_type=jnp.float32)
    live = (jnp.arange(edges.shape[0]) < count).astype(edges.dtype)[:, None]
    edge_new = edges + live * layer_norm(second, egain)
    message = (live * edge_new).astype(jnp.bfloat16)
    gathered = jax.ops.segment_sum(message.astype(edges.dtype), receiving, num_segments=cells.shape[0])
    stacked = jnp.concatenate([cells.astype(jnp.bfloat16), gathered.astype(jnp.bfloat16)], axis=1)
    hidden = jnp.dot(stacked, nw1.astype(jnp.bfloat16), preferred_element_type=jnp.float32)
    output = jnp.dot(jax.nn.silu(hidden).astype(jnp.bfloat16), nw2.astype(jnp.bfloat16), preferred_element_type=jnp.float32)
    return (cells + layer_norm(output, ngain), edge_new)

def build_ghosts(cells_all, rows):
    offsets = (-(N_MORTON // 2), -1, 1, N_MORTON // 2)
    groups = []
    for k in range(4):
        shift_by = offsets[k]
        picked = jnp.take_along_axis(cells_all, rows[:, k, :, None], axis=1)
        blank = jnp.zeros((abs(shift_by),) + picked.shape[1:], cells_all.dtype)
        if shift_by > 0:
            moved = jnp.concatenate([blank, picked[:-shift_by]], axis=0)
        else:
            moved = jnp.concatenate([picked[-shift_by:], blank], axis=0)
        groups.append(moved)
    return jnp.concatenate(groups, axis=1)

def reference(node_feat, edge_feat, cot_node, cot_edge, senders, receivers, send_rows, edge_count, edge_w1, edge_w2, edge_gain, node_w1, node_w2, node_gain):
    weights = (edge_w1, edge_w2, edge_gain, node_w1, node_w2, node_gain)
    grad_nodes = []
    grad_edges = []
    totals = None
    for block in range(BLOCKS):
        cells_all = node_feat[block].astype(jnp.float32).reshape(N_MORTON, C_DEV, H)
        edges_all = edge_feat[block].astype(jnp.float32).reshape(N_MORTON, E_DEV, H)
        sending = senders[block].reshape(N_MORTON, E_DEV)
        receiving = receivers[block].reshape(N_MORTON, E_DEV)
        rows = send_rows[block].reshape(N_MORTON, 4, GQ)
        counts = edge_count[block]

        def whole(cells_all, edges_all, ew1, ew2, egain, nw1, nw2, ngain):
            ghosts = build_ghosts(cells_all, rows)

            def single(items):
                cells, ghost, edges, snd, rcv, cnt = items
                return local_forward(cells, ghost, edges, ew1, ew2, egain, nw1, nw2, ngain, snd, rcv, cnt)
            return lax.map(jax.checkpoint(single), (cells_all, ghosts, edges_all, sending, receiving, counts))
        outputs, pullback = jax.vjp(whole, cells_all, edges_all, *weights)
        cotangents = (cot_node[block].astype(jnp.float32).reshape(N_MORTON, C_DEV, H), cot_edge[block].astype(jnp.float32).reshape(N_MORTON, E_DEV, H))
        grads = pullback(cotangents)
        grad_nodes.append(grads[0].reshape(CELLS, H))
        grad_edges.append(grads[1].reshape(EDGES, H))
        if totals is None:
            totals = grads[2:]
        else:
            totals = tuple((a + b for a, b in zip(totals, grads[2:])))
    factor = 1.0 / jnp.sqrt(jnp.float32(BLOCKS * N_MORTON * E_DEV))
    scaled = tuple((t * factor for t in totals))
    return (jnp.stack(grad_nodes), jnp.stack(grad_edges), scaled[0], scaled[1], scaled[2], scaled[3], scaled[4], scaled[5])
```

```python
import functools

import jax
import jax.numpy as jnp
from jax import lax
from jax.experimental import pallas as pl
from jax.experimental.pallas import tpu as pltpu
from jax.sharding import PartitionSpec as P

BF = jnp.bfloat16
F32 = jnp.float32
EPS = 1e-05
CHUNK = 256


def mm(a, b):
    return lax.dot_general(a, b, (((1,), (0,)), ((), ())), preferred_element_type=F32)


def mm_rt(a, b):
    return lax.dot_general(a, b, (((1,), (1,)), ((), ())), preferred_element_type=F32)


def mm_lt(a, b):
    return lax.dot_general(a, b, (((0,), (0,)), ((), ())), preferred_element_type=F32)


def silu_parts(a):
    sig = 0.5 * jnp.tanh(0.5 * a) + 0.5
    act = a * sig
    return act, sig + act * (1.0 - sig)


def norm_parts(b):
    center = b - jnp.mean(b, axis=-1, keepdims=True)
    inv = lax.rsqrt(jnp.mean(center * center, axis=-1, keepdims=True) + EPS)
    return center * inv, inv


def norm_back(g, nrm, inv):
    return inv * (
        g
        - jnp.mean(g, axis=-1, keepdims=True)
        - nrm * jnp.mean(g * nrm, axis=-1, keepdims=True)
    )


def one_hot_cols(col, size):
    lane = lax.broadcasted_iota(jnp.int32, (col.shape[0], size), 1)
    return jnp.where(jnp.tile(col, (1, size // col.shape[1])) == lane, 1.0, 0.0).astype(BF)


def one_hot_rows(row, size):
    sub = lax.broadcasted_iota(jnp.int32, (size, row.shape[1]), 0)
    return jnp.where(row == sub, 1.0, 0.0).astype(BF)


def layer_kernel(
    count_ref, h_ref, gh_ref, e_ref, cn_ref, ce_ref, snd_ref, rcv_ref,
    w1_ref, w2_ref, eg_ref, nw1_ref, nw2_ref, ng_ref,
    gnode_ref, gedge_ref, gghost_ref, wg_ref,
    tmat, col_s, col_r, rhs, p_s, dsil_s, nrm_s, inv_s, ptr, pts, pr, agg, dagg_s, db_s, da_s,
):
    H = h_ref.shape[1]
    C = h_ref.shape[0]
    E = e_ref.shape[0]
    T = C + gh_ref.shape[0]
    count = count_ref[0, 0]
    nrow = E // 128

    tmat[...] = jnp.zeros_like(tmat)
    for r in range(nrow):
        tmat[r : r + 1, :] = snd_ref[:, r * 128 : (r + 1) * 128]
        tmat[nrow + r : nrow + r + 1, :] = rcv_ref[:, r * 128 : (r + 1) * 128]
    turned = jnp.transpose(tmat[...])
    for r in range(nrow):
        col_s[r * 128 : (r + 1) * 128, :] = jnp.broadcast_to(turned[:, r : r + 1], (128, 128))
        col_r[r * 128 : (r + 1) * 128, :] = jnp.broadcast_to(
            turned[:, nrow + r : nrow + r + 1], (128, 128)
        )

    w1 = w1_ref[...].astype(BF)
    w1e, w1s, w1r = w1[:H], w1[H : 2 * H], w1[2 * H :]
    w2 = w2_ref[...].astype(BF)
    h = h_ref[...]
    rhs[0:H, :] = w1e
    rhs[H : H + C, :] = mm(h, w1s).astype(BF)
    rhs[H + C : H + T, :] = mm(gh_ref[...], w1s).astype(BF)
    rhs[H + T :, :] = mm(h, w1r).astype(BF)
    egain = eg_ref[...]
    agg[...] = jnp.zeros_like(agg)

    def fwd(i, carry):
        at = pl.ds(pl.multiple_of(i * CHUNK, CHUNK), CHUNK)
        e = e_ref[at, :]
        ps = one_hot_cols(col_s[at, :], T)
        p_r = one_hot_cols(col_r[at, :], C)
        pr[at, :] = p_r
        a = mm(jnp.concatenate([e, ps, p_r], axis=1), rhs[...])
        act, dsil = silu_parts(a)
        p = act.astype(BF)
        p_s[at, :] = p
        dsil_s[at, :] = dsil
        nrm, inv = norm_parts(mm(p, w2))
        nrm_s[at, :] = nrm
        inv_s[at, :] = inv
        rowid = lax.broadcasted_iota(jnp.int32, (CHUNK, H), 0) + i * CHUNK
        msg = jnp.where(rowid < count, e.astype(F32) + nrm * egain, 0.0).astype(BF)
        pt_r = one_hot_rows(rcv_ref[:, at], C)
        ptr[:, at] = pt_r
        pts[:, at] = one_hot_rows(snd_ref[:, at], T)
        agg[...] += mm(pt_r, msg)
        return carry

    lax.fori_loop(0, E // CHUNK, fwd, 0)

    nw1 = nw1_ref[...].astype(BF)
    nw2 = nw2_ref[...].astype(BF)
    cn = cn_ref[...].astype(F32)
    aggb = agg[...].astype(BF)
    y = jnp.concatenate([h, aggb], axis=1)
    act, dsil = silu_parts(mm(y, nw1))
    r = act.astype(BF)
    nrm, inv = norm_parts(mm(r, nw2))
    ds = norm_back(cn * ng_ref[...], nrm, inv).astype(BF)
    dc = (mm_rt(ds, nw2) * dsil).astype(BF)
    dy = mm_rt(dc, nw1)
    dagg_s[...] = dy[:, H:].astype(BF)
    gnode_ref[...] = cn + dy[:, :H]
    wg_ref[4 * H : 6 * H, :] = mm_lt(y, dc)
    wg_ref[6 * H : 7 * H, :] = mm_lt(r, ds)
    wg_ref[7 * H :, :] = jnp.zeros((wg_ref.shape[0] - 7 * H, H), F32)
    wg_ref[7 * H + 8 : 7 * H + 9, :] = jnp.sum(cn * nrm, axis=0, keepdims=True)

    def bwd(i, gain_sum):
        at = pl.ds(pl.multiple_of(i * CHUNK, CHUNK), CHUNK)
        dmsg = mm(pr[at, :], dagg_s[...])
        rowid = lax.broadcasted_iota(jnp.int32, (CHUNK, H), 0) + i * CHUNK
        alive = rowid < count
        ce = ce_ref[at, :].astype(F32)
        full = ce + dmsg
        d = jnp.where(alive, full, 0.0)
        nrm = nrm_s[at, :]
        gain_sum = gain_sum + jnp.sum((d * nrm).reshape(CHUNK // 8, 8, H), axis=0)
        db = norm_back(d * egain, nrm, inv_s[at, :]).astype(BF)
        db_s[at, :] = db
        da = (mm_rt(db, w2) * dsil_s[at, :]).astype(BF)
        da_s[at, :] = da
        gedge_ref[at, :] = jnp.where(alive, full, ce) + mm_rt(da, w1e)
        return gain_sum

    gain_sum = lax.fori_loop(0, E // CHUNK, bwd, jnp.zeros((8, H), F32))
    wg_ref[7 * H : 7 * H + 1, :] = jnp.sum(gain_sum, axis=0, keepdims=True)
    da = da_s[...]
    wg_ref[3 * H : 4 * H, :] = mm_lt(p_s[...], db_s[...])
    wg_ref[0:H, :] = mm_lt(e_ref[...], da)
    gs = mm(pts[...], da).astype(BF)
    gr = mm(ptr[...], da).astype(BF)
    table = jnp.concatenate([h, gh_ref[...]], axis=0)
    wg_ref[H : 2 * H, :] = mm_lt(table, gs)
    wg_ref[2 * H : 3 * H, :] = mm_lt(h, gr)
    dt = mm_rt(gs, w1s)
    gnode_ref[...] += dt[:C] + mm_rt(gr, w1r)
    gghost_ref[...] = dt[C:].astype(BF)


def run_layer(count, h, ghosts, e, cn, ce, snd, rcv, ew1, ew2, eg, nw1, nw2, ng, rows):
    C, H = h.shape
    E = e.shape[0]
    G = ghosts.shape[0]
    T = C + G
    vm = pl.BlockSpec(memory_space=pltpu.VMEM)
    shapes = (
        jax.ShapeDtypeStruct((C, H), F32),
        jax.ShapeDtypeStruct((E, H), F32),
        jax.ShapeDtypeStruct((G, H), BF),
        jax.ShapeDtypeStruct((rows, H), F32),
    )
    scratch = [
        pltpu.VMEM((128, 128), jnp.int32),
        pltpu.VMEM((E, 128), jnp.int32),
        pltpu.VMEM((E, 128), jnp.int32),
        pltpu.VMEM((H + T + C, H), BF),
        pltpu.VMEM((E, H), BF),
        pltpu.VMEM((E, H), F32),
        pltpu.VMEM((E, H), F32),
        pltpu.VMEM((E, 1), F32),
        pltpu.VMEM((C, E), BF),
        pltpu.VMEM((T, E), BF),
        pltpu.VMEM((E, C), BF),
        pltpu.VMEM((C, H), F32),
        pltpu.VMEM((C, H), BF),
        pltpu.VMEM((E, H), BF),
        pltpu.VMEM((E, H), BF),
    ]
    return pl.pallas_call(
        layer_kernel,
        out_shape=shapes,
        in_specs=[pl.BlockSpec(memory_space=pltpu.SMEM)] + [vm] * 13,
        out_specs=(vm,) * 4,
        scratch_shapes=scratch,
        compiler_params=pltpu.CompilerParams(vmem_limit_bytes=40 * 1024 * 1024),
        cost_estimate=pl.CostEstimate(
            flops=2 * E * H * 4608, bytes_accessed=6 * E * H * 2, transcendentals=E * H
        ),
        name="mesh_layer",
    )(count, h, ghosts, e, cn, ce, snd, rcv, ew1, ew2, eg, nw1, nw2, ng)


def flip(x, axis, by):
    n = lax.axis_size(axis)
    return lax.ppermute(x, axis, [(i, i ^ by) for i in range(n)])


def pick(x, k):
    return lax.dynamic_index_in_dim(x, k, 0, keepdims=False)


def tree_sum(parts):
    while len(parts) > 1:
        parts = [parts[i] + parts[i + 1] for i in range(0, len(parts), 2)]
    return parts[0]


def scatter_sum(v, axis, stride, width):
    j = lax.axis_index(axis) // stride % width
    pieces = v.astype(BF).reshape(width, v.shape[0] // width, v.shape[1])
    own = pick(pieces, j)
    parts = [own.astype(F32)]
    for d in range(1, width):
        parts.append(flip(pick(pieces, j ^ d), axis, d * stride).astype(F32))
    return tree_sum(parts)


def exchange_sum(v, axis, stride, width):
    w = v.astype(BF)
    parts = [w.astype(F32)]
    for d in range(1, width):
        parts.append(flip(w, axis, d * stride).astype(F32))
    return tree_sum(parts)


def gather_pieces(w, axis, stride, width):
    j = lax.axis_index(axis) // stride % width
    parts = [w] + [flip(w, axis, d * stride) for d in range(1, width)]
    stacked = jnp.stack(parts)
    return jnp.concatenate([pick(stacked, j ^ k) for k in range(width)], axis=0)


def widths(n):
    out = []
    stride = 1
    while stride < n:
        w = 4 if n // stride >= 4 else 2
        out.append((stride, w))
        stride *= w
    return out


def reduce_all(v):
    n = lax.axis_size("morton")
    pair = lax.axis_size("dp")
    stages = widths(n)
    v = scatter_sum(v, "dp", 1, pair)
    v = scatter_sum(v, "morton", *stages[0])
    for stride, width in stages[1:]:
        v = exchange_sum(v, "morton", stride, width)
    w = gather_pieces(v.astype(BF), "morton", *stages[0])
    return gather_pieces(w, "dp", 1, pair).astype(F32)


def on_device(
    node_feat, edge_feat, cot_node, cot_edge, senders, receivers, send_rows, edge_count,
    edge_w1, edge_w2, edge_gain, node_w1, node_w2, node_gain,
):
    peers = lax.axis_size("morton")
    rank = lax.axis_index("morton")
    H = node_feat.shape[2]
    h = node_feat[0]
    C = h.shape[0]
    quota = send_rows.shape[1] // 4
    groups = send_rows[0].reshape(4, quota)
    upper = rank >= peers // 2
    far = jnp.where(upper, groups[0], groups[3])
    rows_out = jnp.concatenate([far, groups[1], groups[2]])
    ids = jnp.arange(C, dtype=jnp.int32)
    picked = jnp.dot(
        (rows_out[:, None] == ids[None, :]).astype(BF), h, preferred_element_type=F32
    ).astype(BF)
    half = peers // 2
    down = [(i, (i - 1) % peers) for i in range(peers)]
    up = [(i, (i + 1) % peers) for i in range(peers)]
    across = [(i, (i + half) % peers) for i in range(peers)]
    from_far = lax.ppermute(picked[:quota], "morton", across)
    from_up = lax.ppermute(picked[quota : 2 * quota], "morton", down)
    from_down = lax.ppermute(picked[2 * quota :], "morton", up)
    ghosts = jnp.concatenate([from_far, from_up, from_down, from_far], axis=0)

    rows = -(-(7 * H + 16) // 64) * 64
    gnode, gedge, gghost, wg = run_layer(
        edge_count, h, ghosts, edge_feat[0], cot_node[0], cot_edge[0], senders, receivers,
        edge_w1, edge_w2, edge_gain.reshape(1, H), node_w1, node_w2, node_gain.reshape(1, H), rows,
    )
    gg = gghost.reshape(4, quota, H)
    back_far = jnp.where(upper, gg[3], gg[0])
    ret_far = lax.ppermute(back_far, "morton", across)
    ret_down = lax.ppermute(gg[1], "morton", up)
    ret_up = lax.ppermute(gg[2], "morton", down)
    returned = jnp.concatenate([ret_far, ret_down, ret_up], axis=0)
    grad_node = gnode + jnp.dot(
        (ids[:, None] == rows_out[None, :]).astype(BF), returned, preferred_element_type=F32
    )

    total = lax.axis_size("dp") * peers * edge_feat.shape[1]
    wsum = reduce_all(wg) * (1.0 / jnp.sqrt(jnp.float32(total)))
    return (
        grad_node[None],
        gedge[None],
        wsum[0 : 3 * H],
        wsum[3 * H : 4 * H],
        wsum[7 * H],
        wsum[4 * H : 6 * H],
        wsum[6 * H : 7 * H],
        wsum[7 * H + 8],
    )


def solution(mesh):
    cells = P("dp", "morton", None)
    flat = P("dp", "morton")
    in_specs = (cells,) * 4 + (flat,) * 4 + (P(),) * 6
    out_specs = (cells, cells) + (P(),) * 6
    return jax.shard_map(
        on_device, mesh=mesh, in_specs=in_specs, out_specs=out_specs, check_vma=False
    )
```

```python
import functools

import jax
import jax.numpy as jnp
from jax import lax
from jax.experimental import pallas as pl
from jax.experimental.pallas import tpu as pltpu
from jax.sharding import PartitionSpec as P

BF = jnp.bfloat16
F32 = jnp.float32
EPS = 1e-05
PRE_CHUNK = 1024
FWD_CHUNK = 2048
BWD_CHUNK = 2048


def mm(a, b):
    return lax.dot_general(a, b, (((1,), (0,)), ((), ())), preferred_element_type=F32)


def mm_rt(a, b):
    return lax.dot_general(a, b, (((1,), (1,)), ((), ())), preferred_element_type=F32)


def mm_lt(a, b):
    return lax.dot_general(a, b, (((0,), (0,)), ((), ())), preferred_element_type=F32)


def silu_parts(a):
    sig = 0.5 * jnp.tanh(0.5 * a) + 0.5
    act = a * sig
    return act, sig + act * (1.0 - sig)


def norm_parts(b):
    center = b - jnp.mean(b, axis=-1, keepdims=True)
    inv = lax.rsqrt(jnp.mean(center * center, axis=-1, keepdims=True) + EPS)
    return center * inv, inv


def norm_back(g, nrm, inv):
    return inv * (
        g
        - jnp.mean(g, axis=-1, keepdims=True)
        - nrm * jnp.mean(g * nrm, axis=-1, keepdims=True)
    )


def one_hot_cols(col, size):
    lane = lax.broadcasted_iota(jnp.int32, (col.shape[0], size), 1)
    return jnp.where(jnp.tile(col, (1, size // col.shape[1])) == lane, 1.0, 0.0).astype(BF)


def one_hot_rows(row, size):
    sub = lax.broadcasted_iota(jnp.int32, (size, row.shape[1]), 0)
    return jnp.where(row == sub, 1.0, 0.0).astype(BF)


def my_place():
    j = lax.axis_index("morton")
    return (j >= lax.axis_size("morton") // 2).astype(jnp.int32), j % 2


def start_all(pairs, sems):
    copies = [pltpu.make_async_copy(src, dst, sems.at[i]) for i, (src, dst) in enumerate(pairs)]
    for c in copies:
        c.start()
    return copies


def spread(row_refs, tmat, outs):
    tmat[...] = jnp.zeros_like(tmat)
    at = 0
    for ref in row_refs:
        for r in range(ref.shape[1] // 128):
            tmat[at : at + 1, :] = ref[:, r * 128 : (r + 1) * 128]
            at += 1
    turned = jnp.transpose(tmat[...])
    at = 0
    for ref, out in zip(row_refs, outs):
        for r in range(ref.shape[1] // 128):
            out[r * 128 : (r + 1) * 128, :] = jnp.broadcast_to(turned[:, at : at + 1], (128, 128))
            at += 1


def pack_kernel(rows_hbm, h_hbm, far_ref, one_ref, two_ref, rows_s, h_s, tmat, col, got, sems):
    copies = start_all([(rows_hbm, rows_s), (h_hbm, h_s)], sems)
    copies[0].wait()
    spread([rows_s], tmat, [col])
    hot = one_hot_cols(col[...], h_s.shape[0])
    copies[1].wait()
    got[...] = mm(hot, h_s[...])
    upper, odd = my_place()
    q = far_ref.shape[0]
    far_ref[...] = got[pl.ds(pl.multiple_of((1 - upper) * 3 * q, q), q), :].astype(BF)
    one_ref[...] = got[pl.ds(pl.multiple_of((2 - odd) * q, q), q), :].astype(BF)
    two_ref[...] = got[pl.ds(pl.multiple_of((1 + odd) * q, q), q), :].astype(BF)


def pre_kernel(
    h_hbm, e_hbm, snd_hbm, rcv_hbm, w1_hbm,
    part_ref, pg_ref, pr_ref, ptr_ref, pts_ref,
    h_s, e_s, snd_s, rcv_s, w1_s, tmat, col_s, col_r, rhs, sems,
):
    copies = start_all(
        [(snd_hbm, snd_s), (rcv_hbm, rcv_s), (h_hbm, h_s), (w1_hbm, w1_s), (e_hbm, e_s)], sems
    )
    C, H = h_s.shape
    E = e_s.shape[0]
    G = pg_ref.shape[1]
    copies[0].wait()
    copies[1].wait()
    spread([snd_s, rcv_s], tmat, [col_s, col_r])
    copies[2].wait()
    copies[3].wait()
    w1 = w1_s[...].astype(BF)
    h = h_s[...]
    rhs[0:H, :] = w1[:H]
    rhs[H : H + C, :] = mm(h, w1[H : 2 * H]).astype(BF)
    rhs[H + C :, :] = mm(h, w1[2 * H :]).astype(BF)
    copies[4].wait()

    def step(i, carry):
        at = pl.ds(pl.multiple_of(i * PRE_CHUNK, PRE_CHUNK), PRE_CHUNK)
        hot = one_hot_cols(col_s[at, :], C + G)
        p_r = one_hot_cols(col_r[at, :], C)
        pg_ref[at, :] = hot[:, C:]
        pr_ref[at, :] = p_r
        part_ref[at, :] = mm(jnp.concatenate([e_s[at, :], hot[:, :C], p_r], axis=1), rhs[...])
        ptr_ref[:, at] = one_hot_rows(rcv_s[:, at], C)
        pts_ref[:, at] = one_hot_rows(snd_s[:, at], C + G)
        return carry

    lax.fori_loop(0, E // PRE_CHUNK, step, 0)


def main_kernel(
    count_ref, part_ref, pg_ref, pr_ref, ptr_ref, pts_ref, far_ref, one_ref, two_ref,
    h_hbm, e_hbm, cn_hbm, ce_hbm, w1_hbm, w2_hbm, eg_hbm, nw1_hbm, nw2_hbm, ng_hbm,
    gnode_ref, gedge_hbm, bfar_ref, bone_ref, btwo_ref, wmine_ref, woth_ref,
    h_s, e_s, cn_s, ce_s, w1_s, w2_s, eg_s, nw1_s, nw2_s, ng_s,
    gh_s, p_s, dsil_s, nrm_s, inv_s, agg, dagg_s, db_s, da_s, gedge_s, wg, dgh, sems, out_sems,
):
    copies = start_all(
        [
            (w1_hbm, w1_s), (w2_hbm, w2_s), (eg_hbm, eg_s), (e_hbm, e_s), (h_hbm, h_s),
            (nw1_hbm, nw1_s), (nw2_hbm, nw2_s), (ng_hbm, ng_s), (cn_hbm, cn_s), (ce_hbm, ce_s),
        ],
        sems,
    )
    C, H = h_s.shape
    E = e_s.shape[0]
    G = pg_ref.shape[1]
    q = G // 4
    count = count_ref[0, 0]
    upper, odd = my_place()
    gh_s[0:q, :] = far_ref[...]
    gh_s[3 * q :, :] = far_ref[...]
    gh_s[pl.ds(pl.multiple_of((1 + odd) * q, q), q), :] = one_ref[...]
    gh_s[pl.ds(pl.multiple_of((2 - odd) * q, q), q), :] = two_ref[...]
    for c in copies[:4]:
        c.wait()
    w1 = w1_s[...].astype(BF)
    w1e, w1s, w1r = w1[:H], w1[H : 2 * H], w1[2 * H :]
    w2 = w2_s[...].astype(BF)
    egain = eg_s[...]
    gtab = mm(gh_s[...], w1s).astype(BF)
    agg[...] = jnp.zeros_like(agg)

    def fwd(i, carry):
        at = pl.ds(pl.multiple_of(i * FWD_CHUNK, FWD_CHUNK), FWD_CHUNK)
        act, dsil = silu_parts(part_ref[at, :] + mm(pg_ref[at, :], gtab))
        p = act.astype(BF)
        p_s[at, :] = p
        dsil_s[at, :] = dsil
        nrm, inv = norm_parts(mm(p, w2))
        nrm_s[at, :] = nrm
        inv_s[at, :] = inv
        rowid = lax.broadcasted_iota(jnp.int32, (FWD_CHUNK, H), 0) + i * FWD_CHUNK
        msg = jnp.where(rowid < count, e_s[at, :].astype(F32) + nrm * egain, 0.0).astype(BF)
        agg[...] += mm(ptr_ref[:, at], msg)
        return carry

    lax.fori_loop(0, E // FWD_CHUNK, fwd, 0)

    for c in copies[4:]:
        c.wait()
    h = h_s[...]
    nw1 = nw1_s[...].astype(BF)
    nw2 = nw2_s[...].astype(BF)
    cn = cn_s[...].astype(F32)
    aggb = agg[...].astype(BF)
    y = jnp.concatenate([h, aggb], axis=1)
    act, dsil = silu_parts(mm(y, nw1))
    r = act.astype(BF)
    nrm, inv = norm_parts(mm(r, nw2))
    ds = norm_back(cn * ng_s[...], nrm, inv).astype(BF)
    dc = (mm_rt(ds, nw2) * dsil).astype(BF)
    dy = mm_rt(dc, nw1)
    dagg_s[...] = dy[:, H:].astype(BF)
    gnode_ref[...] = cn + dy[:, :H]
    wg[4 * H : 6 * H, :] = mm_lt(y, dc)
    wg[6 * H : 7 * H, :] = mm_lt(r, ds)
    wg[7 * H :, :] = jnp.zeros((wg.shape[0] - 7 * H, H), F32)
    wg[7 * H + 8 : 7 * H + 9, :] = jnp.sum(cn * nrm, axis=0, keepdims=True)

    def out_copy(i):
        at = pl.ds(pl.multiple_of(i * BWD_CHUNK, BWD_CHUNK), BWD_CHUNK)
        return pltpu.make_async_copy(gedge_s.at[at, :], gedge_hbm.at[at, :], out_sems.at[i])

    gain_sum = jnp.zeros((8, H), F32)
    for i in range(E // BWD_CHUNK):
        at = pl.ds(i * BWD_CHUNK, BWD_CHUNK)
        dmsg = mm(pr_ref[at, :], dagg_s[...])
        rowid = lax.broadcasted_iota(jnp.int32, (BWD_CHUNK, H), 0) + i * BWD_CHUNK
        alive = rowid < count
        ce = ce_s[at, :].astype(F32)
        full = ce + dmsg
        d = jnp.where(alive, full, 0.0)
        nrm = nrm_s[at, :]
        gain_sum = gain_sum + jnp.sum((d * nrm).reshape(BWD_CHUNK // 8, 8, H), axis=0)
        db = norm_back(d * egain, nrm, inv_s[at, :]).astype(BF)
        db_s[at, :] = db
        da = (mm_rt(db, w2) * dsil_s[at, :]).astype(BF)
        da_s[at, :] = da
        gedge_s[at, :] = jnp.where(alive, full, ce) + mm_rt(da, w1e)
        out_copy(i).start()

    wg[7 * H : 7 * H + 1, :] = jnp.sum(gain_sum, axis=0, keepdims=True)
    da = da_s[...]
    gs = mm(pts_ref[...], da).astype(BF)
    gr = mm(ptr_ref[...], da).astype(BF)
    wg[3 * H : 4 * H, :] = mm_lt(p_s[...], db_s[...])
    wg[0:H, :] = mm_lt(e_s[...], da)
    wg[H : 2 * H, :] = mm_lt(jnp.concatenate([h, gh_s[...]], axis=0), gs)
    wg[2 * H : 3 * H, :] = mm_lt(h, gr)
    dt = mm_rt(gs, w1s)
    gnode_ref[...] += dt[:C] + mm_rt(gr, w1r)
    dgh[...] = dt[C:]
    bfar_ref[...] = dgh[pl.ds(pl.multiple_of(upper * 3 * q, q), q), :].astype(BF)
    bone_ref[...] = dgh[pl.ds(pl.multiple_of((1 + odd) * q, q), q), :].astype(BF)
    btwo_ref[...] = dgh[pl.ds(pl.multiple_of((2 - odd) * q, q), q), :].astype(BF)
    core = lax.axis_index("dp")
    part = wmine_ref.shape[0]
    wmine_ref[...] = wg[pl.ds(pl.multiple_of(core * part, 8), part), :].astype(BF)
    woth_ref[...] = wg[pl.ds(pl.multiple_of((1 - core) * part, 8), part), :].astype(BF)
    for i in range(E // BWD_CHUNK):
        out_copy(i).wait()


def node_kernel(rows_hbm, gnode_ref, far_ref, one_ref, two_ref, out_ref, rows_s, ret, sems):
    copies = start_all([(rows_hbm, rows_s)], sems)
    upper, odd = my_place()
    q = far_ref.shape[0]
    ret[...] = jnp.zeros_like(ret)
    ret[pl.ds(pl.multiple_of((1 - upper) * 3 * q, q), q), :] = far_ref[...]
    ret[pl.ds(pl.multiple_of((2 - odd) * q, q), q), :] = one_ref[...]
    ret[pl.ds(pl.multiple_of((1 + odd) * q, q), q), :] = two_ref[...]
    copies[0].wait()
    out_ref[...] = gnode_ref[...] + mm(one_hot_rows(rows_s[...], out_ref.shape[0]), ret[...])


def unpack_kernel(factor, mine_ref, oth_ref, g1, g2, gg, gn1, gn2, gng, wg):
    core = lax.axis_index("dp")
    part, H = mine_ref.shape
    wg[pl.ds(pl.multiple_of(core * part, 8), part), :] = mine_ref[...].astype(F32) * factor
    wg[pl.ds(pl.multiple_of((1 - core) * part, 8), part), :] = oth_ref[...].astype(F32) * factor
    g1[...] = wg[0 : 3 * H, :]
    g2[...] = wg[3 * H : 4 * H, :]
    gn1[...] = wg[4 * H : 6 * H, :]
    gn2[...] = wg[6 * H : 7 * H, :]
    gg[...] = wg[7 * H : 7 * H + 1, :]
    gng[...] = wg[7 * H + 8 : 7 * H + 9, :]


HBM = pl.BlockSpec(memory_space=pltpu.HBM)
VM = pl.BlockSpec(memory_space=pltpu.VMEM)
SM = pl.BlockSpec(memory_space=pltpu.SMEM)
MIB = 1024 * 1024


def like(x):
    return pltpu.VMEM(x.shape, x.dtype)


def sds(shape, dtype):
    return jax.ShapeDtypeStruct(shape, dtype)


def call(kernel, name, outs, in_specs, out_specs, scratch, flops, nbytes, limit):
    return pl.pallas_call(
        kernel,
        out_shape=outs,
        in_specs=in_specs,
        out_specs=out_specs,
        scratch_shapes=scratch,
        compiler_params=pltpu.CompilerParams(vmem_limit_bytes=limit * MIB),
        cost_estimate=pl.CostEstimate(flops=flops, bytes_accessed=nbytes, transcendentals=0),
        name=name,
    )


def flip(x, axis, by):
    n = lax.axis_size(axis)
    return lax.ppermute(x, axis, [(i, i ^ by) for i in range(n)])


def cross_pairs(x):
    n = lax.axis_size("morton")
    return lax.ppermute(x, "morton", [(i, (i + 1) % n if i % 2 else (i - 1) % n) for i in range(n)])


def pick(x, k):
    return lax.dynamic_index_in_dim(x, k, 0, keepdims=False)


def tree_sum(parts):
    while len(parts) > 1:
        parts = [parts[i] + parts[i + 1] for i in range(0, len(parts), 2)]
    return parts[0]


def stages_of(n):
    out = []
    stride = 1
    while stride < n:
        w = 4 if n // stride >= 4 else 2
        out.append((stride, w))
        stride *= w
    return out


def flip_with(x, by, extra, got):
    if by in extra:
        rider = extra.pop(by)
        moved = flip(jnp.concatenate([x, rider], axis=0), "morton", by)
        got[by] = moved[x.shape[0] :]
        return moved[: x.shape[0]]
    return flip(x, "morton", by)


def reduce_all(mine, oth, extra, early, finish):
    got = {}
    stages = stages_of(lax.axis_size("morton"))
    v = mine.astype(F32) + flip(oth, "dp", 1).astype(F32)
    stride, width = stages[0]
    j = lax.axis_index("morton") % width
    pieces = v.astype(BF).reshape(width, v.shape[0] // width, v.shape[1])
    parts = [pick(pieces, j).astype(F32)]
    for d in range(1, width):
        parts.append(flip_with(pick(pieces, j ^ d), d, extra, got).astype(F32))
    v, early = lax.optimization_barrier((tree_sum(parts), early))
    for stride, width in stages[1:]:
        w = v.astype(BF)
        parts = [w.astype(F32)]
        for d in range(1, width):
            parts.append(flip_with(w, d * stride, extra, got).astype(F32))
        v = tree_sum(parts)
    for by in list(extra):
        got[by] = flip(extra.pop(by), "morton", by)
    w = v.astype(BF)
    stacked = jnp.stack([w] + [flip(w, "morton", d) for d in range(1, stages[0][1])])
    mine = jnp.concatenate([pick(stacked, j ^ k) for k in range(stages[0][1])], axis=0)
    mine, done = lax.optimization_barrier((mine, finish(early, got)))
    return mine, flip(mine, "dp", 1), done


def on_device(
    node_feat, edge_feat, cot_node, cot_edge, senders, receivers, send_rows, edge_count,
    edge_w1, edge_w2, edge_gain, node_w1, node_w2, node_gain,
):
    peers = lax.axis_size("morton")
    pair = lax.axis_size("dp")
    half = peers // 2
    h, e, cn, ce = node_feat[0], edge_feat[0], cot_node[0], cot_edge[0]
    C, H = h.shape
    E = e.shape[0]
    G = send_rows.shape[1]
    q = G // 4
    T = C + G
    i32 = jnp.int32
    dma = pltpu.SemaphoreType.DMA
    egain, ngain = edge_gain.reshape(1, H), node_gain.reshape(1, H)

    ghost = sds((q, H), BF)
    far, one, two = call(
        pack_kernel, "pack_ghosts", (ghost,) * 3, [HBM] * 2, (VM,) * 3,
        [like(send_rows), like(h), pltpu.VMEM((128, 128), i32), pltpu.VMEM((G, 128), i32),
         pltpu.VMEM((G, H), F32), dma((2,))],
        4_000_000_000, 8_000_000, 8,
    )(send_rows, h)
    far = flip(far, "morton", half)
    one = flip(one, "morton", 1)
    two = cross_pairs(two)

    part, pg, pr, ptr, pts = call(
        pre_kernel, "edge_pre",
        (sds((E, H), F32), sds((E, G), BF), sds((E, C), BF), sds((C, E), BF), sds((T, E), BF)),
        [HBM] * 5, (VM,) * 5,
        [like(h), like(e), like(senders), like(receivers), like(edge_w1),
         pltpu.VMEM((128, 128), i32), pltpu.VMEM((E, 128), i32), pltpu.VMEM((E, 128), i32),
         pltpu.VMEM((H + 2 * C, H), BF), dma((5,))],
        2 * E * H * (H + 2 * C) * 4, 4 * E * (H + T), 24,
    )(h, e, senders, receivers, edge_w1)

    rows = -(-(7 * H + 16) // (pair * 32)) * (pair * 32)
    mine_shape = sds((rows // pair, H), BF)
    hbm_in = [h, e, cn, ce, edge_w1, edge_w2, egain, node_w1, node_w2, ngain]
    gnode, gedge, bfar, bone, btwo, wmine, woth = call(
        main_kernel, "mesh_layer",
        (sds((C, H), F32), sds((E, H), F32), ghost, ghost, ghost, mine_shape, mine_shape),
        [SM] + [VM] * 8 + [HBM] * 10,
        (VM, HBM, VM, VM, VM, VM, VM),
        [like(x) for x in hbm_in]
        + [pltpu.VMEM((G, H), BF), pltpu.VMEM((E, H), BF), pltpu.VMEM((E, H), F32),
           pltpu.VMEM((E, H), F32), pltpu.VMEM((E, 1), F32), pltpu.VMEM((C, H), F32),
           pltpu.VMEM((C, H), BF), pltpu.VMEM((E, H), BF), pltpu.VMEM((E, H), BF),
           pltpu.VMEM((E, H), F32), pltpu.VMEM((rows, H), F32), pltpu.VMEM((G, H), F32),
           dma((10,)), dma((E // BWD_CHUNK,))],
        2 * E * H * 4608, 8 * E * H, 36,
    )(edge_count, part, pg, pr, ptr, pts, far, one, two, *hbm_in)

    def finish(rtwo, got):
        return call(
            node_kernel, "node_grad", sds((C, H), F32), [HBM] + [VM] * 4, VM,
            [like(send_rows), pltpu.VMEM((G, H), BF), dma((1,))],
            2 * C * G * H, 8 * C * H, 8,
        )(send_rows, gnode, got[half], got[1], rtwo)

    mine, oth, grad_node = reduce_all(
        wmine, woth, {1: bone, half: bfar}, cross_pairs(btwo), finish
    )
    factor = float(pair * peers * E) ** -0.5
    g1, g2, gg, gn1, gn2, gng = call(
        functools.partial(unpack_kernel, factor), "weight_grads",
        tuple(sds(s, F32) for s in ((3 * H, H), (H, H), (1, H), (2 * H, H), (H, H), (1, H))),
        [VM] * 2, (VM,) * 6, [pltpu.VMEM((rows, H), F32)], rows * H, 8 * rows * H, 8,
    )(mine, oth)
    return (
        grad_node[None], gedge[None], g1, g2, gg.reshape(H), gn1, gn2, gng.reshape(H),
    )


def solution(mesh):
    cells = P("dp", "morton", None)
    flat = P("dp", "morton")
    in_specs = (cells,) * 4 + (flat,) * 4 + (P(),) * 6
    out_specs = (cells, cells) + (P(),) * 6
    return jax.shard_map(
        on_device, mesh=mesh, in_specs=in_specs, out_specs=out_specs, check_vma=False
    )
```

```python
import functools

import jax
import jax.numpy as jnp
from jax import lax
from jax.experimental import pallas as pl
from jax.experimental.pallas import tpu as pltpu
from jax.sharding import PartitionSpec as P

BF = jnp.bfloat16
F32 = jnp.float32
EPS = 1e-05
PRE_CHUNK = 1024
FWD_CHUNK = 2048
BWD_CHUNK = 2048
LANES = 128


def mm(a, b):
    return lax.dot_general(a, b, (((1,), (0,)), ((), ())), preferred_element_type=F32)


def mm_rt(a, b):
    return lax.dot_general(a, b, (((1,), (1,)), ((), ())), preferred_element_type=F32)


def mm_lt(a, b):
    return lax.dot_general(a, b, (((0,), (0,)), ((), ())), preferred_element_type=F32)


def silu_parts(a):
    sig = 0.5 * jnp.tanh(0.5 * a) + 0.5
    act = a * sig
    return act, sig + act * (1.0 - sig)


def norm_parts(b):
    center = b - jnp.mean(b, axis=-1, keepdims=True)
    inv = lax.rsqrt(jnp.mean(center * center, axis=-1, keepdims=True) + EPS)
    return center * inv, inv


def norm_back(g, nrm, inv):
    return inv * (
        g
        - jnp.mean(g, axis=-1, keepdims=True)
        - nrm * jnp.mean(g * nrm, axis=-1, keepdims=True)
    )


def one_hot_cols(low, high, size):
    lane = lax.broadcasted_iota(jnp.int32, low.shape, 1).astype(F32).astype(BF)
    one, zero = jnp.ones_like(low), jnp.zeros_like(low)
    base = jnp.where(low == lane, one, zero)
    tiles = [jnp.where(high == jnp.full_like(high, t), base, zero) for t in range(size // LANES)]
    return jnp.concatenate(tiles, axis=1)


def one_hot_rows(row, size):
    sub = lax.broadcasted_iota(jnp.int32, (size, row.shape[1]), 0)
    return jnp.where(row == sub, 1.0, 0.0).astype(BF)


def my_place():
    j = lax.axis_index("morton")
    return (j >= lax.axis_size("morton") // 2).astype(jnp.int32), j % 2


def spread(row_refs, tmat, outs):
    tmat[...] = jnp.zeros_like(tmat)
    at = 0
    for ref in row_refs:
        for r in range(ref.shape[1] // LANES):
            tmat[at : at + 1, :] = ref[:, r * LANES : (r + 1) * LANES]
            at += 1
    turned = jnp.transpose(tmat[...])
    low = (turned % LANES).astype(F32).astype(BF)
    high = (turned // LANES).astype(F32).astype(BF)
    at = 0
    for ref, (low_ref, high_ref) in zip(row_refs, outs):
        for r in range(ref.shape[1] // LANES):
            rows = slice(r * LANES, (r + 1) * LANES)
            low_ref[rows, :] = jnp.broadcast_to(low[:, at : at + 1], (LANES, LANES))
            high_ref[rows, :] = jnp.broadcast_to(high[:, at : at + 1], (LANES, LANES))
            at += 1


def pack_kernel(rows_s, h_s, far_ref, one_ref, two_ref, tmat, low, high, got):
    spread([rows_s], tmat, [(low, high)])
    hot = one_hot_cols(low[...], high[...], h_s.shape[0])
    got[...] = mm(hot, h_s[...])
    upper, odd = my_place()
    q = far_ref.shape[0]
    far_ref[...] = got[pl.ds(pl.multiple_of((1 - upper) * 3 * q, q), q), :].astype(BF)
    one_ref[...] = got[pl.ds(pl.multiple_of((2 - odd) * q, q), q), :].astype(BF)
    two_ref[...] = got[pl.ds(pl.multiple_of((1 + odd) * q, q), q), :].astype(BF)


def pre_kernel(
    h_s, e_s, snd_s, rcv_s, w1_s, part_ref, ps_ref, pr_ref, tmat, low_s, high_s, low_r, high_r, rhs
):
    C, H = h_s.shape
    E = e_s.shape[0]
    T = ps_ref.shape[1]
    spread([snd_s, rcv_s], tmat, [(low_s, high_s), (low_r, high_r)])
    w1 = w1_s[...].astype(BF)
    h = h_s[...]
    rhs[0:H, :] = w1[:H]
    rhs[H : H + C, :] = mm(h, w1[H : 2 * H]).astype(BF)
    rhs[H + C :, :] = mm(h, w1[2 * H :]).astype(BF)

    def step(i, carry):
        at = pl.ds(pl.multiple_of(i * PRE_CHUNK, PRE_CHUNK), PRE_CHUNK)
        p_s = one_hot_cols(low_s[at, :], high_s[at, :], T)
        p_r = one_hot_cols(low_r[at, :], high_r[at, :], C)
        ps_ref[at, :] = p_s
        pr_ref[at, :] = p_r
        part_ref[at, :] = mm(jnp.concatenate([e_s[at, :], p_s[:, :C], p_r], axis=1), rhs[...])
        return carry

    lax.fori_loop(0, E // PRE_CHUNK, step, 0)


def main_kernel(
    count_hbm, part_ref, ps_ref, pr_ref, far_ref, one_ref, two_ref,
    h_s, e_s, cn_s, ce_s, w1_s, w2_s, eg_s, nw1_s, nw2_s, ng_s,
    gnode_ref, gedge_hbm, bfar_ref, bone_ref, btwo_ref, wmine_ref, woth_ref,
    gh_s, p_s, dsil_s, nrm_s, inv_s, agg, dagg_s, db_s, da_s, gedge_s, wg, dgh, count_s,
    count_sem, out_sems,
):
    count_copy = pltpu.make_async_copy(count_hbm, count_s, count_sem)
    count_copy.start()
    C, H = h_s.shape
    E = e_s.shape[0]
    G = gh_s.shape[0]
    q = G // 4
    upper, odd = my_place()
    gh_s[0:q, :] = far_ref[...]
    gh_s[3 * q :, :] = far_ref[...]
    gh_s[pl.ds(pl.multiple_of((1 + odd) * q, q), q), :] = one_ref[...]
    gh_s[pl.ds(pl.multiple_of((2 - odd) * q, q), q), :] = two_ref[...]
    w1 = w1_s[...].astype(BF)
    w1e, w1s, w1r = w1[:H], w1[H : 2 * H], w1[2 * H :]
    w2 = w2_s[...].astype(BF)
    egain = eg_s[...]
    gtab = mm(gh_s[...], w1s).astype(BF)
    agg[...] = jnp.zeros_like(agg)
    count_copy.wait()
    count = count_s[0, 0]

    def fwd(i, carry):
        at = pl.ds(pl.multiple_of(i * FWD_CHUNK, FWD_CHUNK), FWD_CHUNK)
        act, dsil = silu_parts(part_ref[at, :] + mm(ps_ref[at, C:], gtab))
        p = act.astype(BF)
        p_s[at, :] = p
        dsil_s[at, :] = dsil
        nrm, inv = norm_parts(mm(p, w2))
        nrm_s[at, :] = nrm
        inv_s[at, :] = inv
        rowid = lax.broadcasted_iota(jnp.int32, (FWD_CHUNK, H), 0) + i * FWD_CHUNK
        msg = jnp.where(rowid < count, e_s[at, :].astype(F32) + nrm * egain, 0.0).astype(BF)
        agg[...] += mm_lt(msg, pr_ref[at, :])
        return carry

    lax.fori_loop(0, E // FWD_CHUNK, fwd, 0)

    h = h_s[...]
    nw1 = nw1_s[...].astype(BF)
    nw2 = nw2_s[...].astype(BF)
    cn = cn_s[...].astype(F32)
    aggb = jnp.transpose(agg[...]).astype(BF)
    y = jnp.concatenate([h, aggb], axis=1)
    act, dsil = silu_parts(mm(y, nw1))
    r = act.astype(BF)
    nrm, inv = norm_parts(mm(r, nw2))
    ds = norm_back(cn * ng_s[...], nrm, inv).astype(BF)
    dc = (mm_rt(ds, nw2) * dsil).astype(BF)
    dy = mm_rt(dc, nw1)
    dagg_s[...] = dy[:, H:].astype(BF)
    gnode_ref[...] = cn + dy[:, :H]
    wg[4 * H : 6 * H, :] = mm_lt(y, dc)
    wg[6 * H : 7 * H, :] = mm_lt(r, ds)
    wg[7 * H :, :] = jnp.zeros((wg.shape[0] - 7 * H, H), F32)
    wg[7 * H + 8 : 7 * H + 9, :] = jnp.sum(cn * nrm, axis=0, keepdims=True)

    def out_copy(i):
        at = pl.ds(pl.multiple_of(i * BWD_CHUNK, BWD_CHUNK), BWD_CHUNK)
        return pltpu.make_async_copy(gedge_s.at[at, :], gedge_hbm.at[at, :], out_sems.at[i])

    gain_sum = jnp.zeros((8, H), F32)
    for i in range(E // BWD_CHUNK):
        at = pl.ds(i * BWD_CHUNK, BWD_CHUNK)
        dmsg = mm(pr_ref[at, :], dagg_s[...])
        rowid = lax.broadcasted_iota(jnp.int32, (BWD_CHUNK, H), 0) + i * BWD_CHUNK
        alive = rowid < count
        ce = ce_s[at, :].astype(F32)
        full = ce + dmsg
        d = jnp.where(alive, full, 0.0)
        nrm = nrm_s[at, :]
        gain_sum = gain_sum + jnp.sum((d * nrm).reshape(BWD_CHUNK // 8, 8, H), axis=0)
        db = norm_back(d * egain, nrm, inv_s[at, :]).astype(BF)
        db_s[at, :] = db
        da = (mm_rt(db, w2) * dsil_s[at, :]).astype(BF)
        da_s[at, :] = da
        gedge_s[at, :] = jnp.where(alive, full, ce) + mm_rt(da, w1e)
        out_copy(i).start()

    wg[7 * H : 7 * H + 1, :] = jnp.sum(gain_sum, axis=0, keepdims=True)
    da = da_s[...]
    gs_t = mm_lt(da, ps_ref[...]).astype(BF)
    gr_t = mm_lt(da, pr_ref[...]).astype(BF)
    table = jnp.concatenate([h, gh_s[...]], axis=0)
    wg[3 * H : 4 * H, :] = mm_lt(p_s[...], db_s[...])
    wg[0:H, :] = jnp.transpose(mm_lt(da, e_s[...]))
    wg[H : 2 * H, :] = jnp.transpose(mm(gs_t, table))
    wg[2 * H : 3 * H, :] = jnp.transpose(mm(gr_t, h))
    dt = jnp.transpose(mm(w1s, gs_t))
    gnode_ref[...] += dt[:C] + jnp.transpose(mm(w1r, gr_t))
    dgh[...] = dt[C:]
    bfar_ref[...] = dgh[pl.ds(pl.multiple_of(upper * 3 * q, q), q), :].astype(BF)
    bone_ref[...] = dgh[pl.ds(pl.multiple_of((1 + odd) * q, q), q), :].astype(BF)
    btwo_ref[...] = dgh[pl.ds(pl.multiple_of((2 - odd) * q, q), q), :].astype(BF)
    core = lax.axis_index("dp")
    part = wmine_ref.shape[0]
    wmine_ref[...] = wg[pl.ds(pl.multiple_of(core * part, 8), part), :].astype(BF)
    woth_ref[...] = wg[pl.ds(pl.multiple_of((1 - core) * part, 8), part), :].astype(BF)
    for i in range(E // BWD_CHUNK):
        out_copy(i).wait()


def node_kernel(rows_s, gnode_ref, far_ref, one_ref, two_ref, out_ref, ret):
    upper, odd = my_place()
    q = far_ref.shape[0]
    ret[...] = jnp.zeros_like(ret)
    ret[pl.ds(pl.multiple_of((1 - upper) * 3 * q, q), q), :] = far_ref[...]
    ret[pl.ds(pl.multiple_of((2 - odd) * q, q), q), :] = one_ref[...]
    ret[pl.ds(pl.multiple_of((1 + odd) * q, q), q), :] = two_ref[...]
    out_ref[...] = gnode_ref[...] + mm(one_hot_rows(rows_s[...], out_ref.shape[0]), ret[...])


def unpack_kernel(factor, mine_ref, oth_ref, g1, g2, gg, gn1, gn2, gng, wg):
    core = lax.axis_index("dp")
    part, H = mine_ref.shape
    wg[pl.ds(pl.multiple_of(core * part, 8), part), :] = mine_ref[...].astype(F32) * factor
    wg[pl.ds(pl.multiple_of((1 - core) * part, 8), part), :] = oth_ref[...].astype(F32) * factor
    g1[...] = wg[0 : 3 * H, :]
    g2[...] = wg[3 * H : 4 * H, :]
    gn1[...] = wg[4 * H : 6 * H, :]
    gn2[...] = wg[6 * H : 7 * H, :]
    gg[...] = wg[7 * H : 7 * H + 1, :]
    gng[...] = wg[7 * H + 8 : 7 * H + 9, :]


HBM = pl.BlockSpec(memory_space=pltpu.HBM)
VM = pl.BlockSpec(memory_space=pltpu.VMEM)
MIB = 1024 * 1024


def sds(shape, dtype):
    return jax.ShapeDtypeStruct(shape, dtype)


def call(kernel, name, outs, in_specs, out_specs, scratch, flops, nbytes, limit):
    return pl.pallas_call(
        kernel,
        out_shape=outs,
        in_specs=in_specs,
        out_specs=out_specs,
        scratch_shapes=scratch,
        compiler_params=pltpu.CompilerParams(vmem_limit_bytes=limit * MIB),
        cost_estimate=pl.CostEstimate(flops=flops, bytes_accessed=nbytes, transcendentals=0),
        name=name,
    )


def flip(x, axis, by):
    n = lax.axis_size(axis)
    return lax.ppermute(x, axis, [(i, i ^ by) for i in range(n)])


def cross_pairs(x):
    n = lax.axis_size("morton")
    return lax.ppermute(x, "morton", [(i, (i + 1) % n if i % 2 else (i - 1) % n) for i in range(n)])


def pick(x, k):
    return lax.dynamic_index_in_dim(x, k, 0, keepdims=False)


def tree_sum(parts):
    while len(parts) > 1:
        parts = [parts[i] + parts[i + 1] for i in range(0, len(parts), 2)]
    return parts[0]


def stages_of(n):
    out = []
    stride = 1
    while stride < n:
        w = 4 if n // stride >= 4 else 2
        out.append((stride, w))
        stride *= w
    return out


def flip_with(x, by, extra, got):
    if by in extra:
        rider = extra.pop(by)
        moved = flip(jnp.concatenate([x, rider], axis=0), "morton", by)
        got[by] = moved[x.shape[0] :]
        return moved[: x.shape[0]]
    return flip(x, "morton", by)


def reduce_all(mine, oth, extra, early, finish):
    got = {}
    stages = stages_of(lax.axis_size("morton"))
    v = mine.astype(F32) + flip(oth, "dp", 1).astype(F32)
    low = lax.axis_index("morton") % 2
    halves = v.astype(BF).reshape(2, v.shape[0] // 2, v.shape[1])
    kept, given = pick(halves, low), pick(halves, 1 - low)
    parts = [kept.astype(F32)]
    for d in range(1, stages[0][1]):
        parts.append(flip_with(given if d % 2 else kept, d, extra, got).astype(F32))
    v, early = lax.optimization_barrier((tree_sum(parts), early))
    for stride, width in stages[1:]:
        w = v.astype(BF)
        parts = [w.astype(F32)]
        for d in range(1, width):
            parts.append(flip_with(w, d * stride, extra, got).astype(F32))
        v = tree_sum(parts)
    for by in list(extra):
        got[by] = flip(extra.pop(by), "morton", by)
    w = v.astype(BF)
    back = flip(w, "morton", 1)
    both = jnp.stack([w, back])
    mine = jnp.concatenate([pick(both, low), pick(both, 1 - low)], axis=0)
    mine, done = lax.optimization_barrier((mine, finish(early, got)))
    return mine, flip(mine, "dp", 1), done


def on_device(
    node_feat, edge_feat, cot_node, cot_edge, senders, receivers, send_rows, edge_count,
    edge_w1, edge_w2, edge_gain, node_w1, node_w2, node_gain,
):
    peers = lax.axis_size("morton")
    pair = lax.axis_size("dp")
    half = peers // 2
    h, e, cn, ce = node_feat[0], edge_feat[0], cot_node[0], cot_edge[0]
    C, H = h.shape
    E = e.shape[0]
    G = send_rows.shape[1]
    q = G // 4
    T = C + G
    i32 = jnp.int32
    dma = pltpu.SemaphoreType.DMA
    egain, ngain = edge_gain.reshape(1, H), node_gain.reshape(1, H)

    ghost = sds((q, H), BF)
    far, one, two = call(
        pack_kernel, "pack_ghosts", (ghost,) * 3, [VM] * 2, (VM,) * 3,
        [pltpu.VMEM((LANES, LANES), i32), pltpu.VMEM((G, LANES), BF),
         pltpu.VMEM((G, LANES), BF), pltpu.VMEM((G, H), F32)],
        4_000_000_000, 8_000_000, 8,
    )(send_rows, h)
    far = flip(far, "morton", half)
    one = flip(one, "morton", 1)
    two = cross_pairs(two)

    part, ps, pr = call(
        pre_kernel, "edge_pre", (sds((E, H), F32), sds((E, T), BF), sds((E, C), BF)),
        [VM] * 5, (VM,) * 3,
        [pltpu.VMEM((LANES, LANES), i32)] + [pltpu.VMEM((E, LANES), BF)] * 4
        + [pltpu.VMEM((H + 2 * C, H), BF)],
        2 * E * H * (H + 2 * C) * 4, 4 * E * (H + T), 24,
    )(h, e, senders, receivers, edge_w1)

    rows = -(-(7 * H + 16) // (pair * 32)) * (pair * 32)
    mine_shape = sds((rows // pair, H), BF)
    layer_in = [h, e, cn, ce, edge_w1, edge_w2, egain, node_w1, node_w2, ngain]
    gnode, gedge, bfar, bone, btwo, wmine, woth = call(
        main_kernel, "mesh_layer",
        (sds((C, H), F32), sds((E, H), F32), ghost, ghost, ghost, mine_shape, mine_shape),
        [HBM] + [VM] * 16,
        (VM, HBM, VM, VM, VM, VM, VM),
        [pltpu.VMEM((G, H), BF), pltpu.VMEM((E, H), BF), pltpu.VMEM((E, H), F32),
           pltpu.VMEM((E, H), F32), pltpu.VMEM((E, 1), F32), pltpu.VMEM((H, C), F32),
           pltpu.VMEM((C, H), BF), pltpu.VMEM((E, H), BF), pltpu.VMEM((E, H), BF),
           pltpu.VMEM((E, H), F32), pltpu.VMEM((rows, H), F32), pltpu.VMEM((G, H), F32),
           pltpu.SMEM((1, 1), i32), dma, dma((E // BWD_CHUNK,))],
        2 * E * H * 4608, 8 * E * H, 36,
    )(edge_count, part, ps, pr, far, one, two, *layer_in)

    def finish(rtwo, got):
        return call(
            node_kernel, "node_grad", sds((C, H), F32), [VM] * 5, VM,
            [pltpu.VMEM((G, H), BF)],
            2 * C * G * H, 8 * C * H, 8,
        )(send_rows, gnode, got[half], got[1], rtwo)

    mine, oth, grad_node = reduce_all(
        wmine, woth, {1: bone, half: bfar}, cross_pairs(btwo), finish
    )
    factor = float(pair * peers * E) ** -0.5
    g1, g2, gg, gn1, gn2, gng = call(
        functools.partial(unpack_kernel, factor), "weight_grads",
        tuple(sds(s, F32) for s in ((3 * H, H), (H, H), (1, H), (2 * H, H), (H, H), (1, H))),
        [VM] * 2, (VM,) * 6, [pltpu.VMEM((rows, H), F32)], rows * H, 8 * rows * H, 8,
    )(mine, oth)
    return (
        grad_node[None], gedge[None], g1, g2, gg.reshape(H), gn1, gn2, gng.reshape(H),
    )


def solution(mesh):
    cells = P("dp", "morton", None)
    flat = P("dp", "morton")
    in_specs = (cells,) * 4 + (flat,) * 4 + (P(),) * 6
    out_specs = (cells, cells) + (P(),) * 6
    return jax.shard_map(
        on_device, mesh=mesh, in_specs=in_specs, out_specs=out_specs, check_vma=False
    )
```

```python
import functools

import jax
import jax.numpy as jnp
from jax import lax
from jax.experimental import pallas as pl
from jax.experimental.pallas import tpu as pltpu
from jax.sharding import PartitionSpec as P


BF = jnp.bfloat16
F32 = jnp.float32
EPS = 1e-05
PRE_CHUNK = 1024
FWD_CHUNK = 2048
BWD_CHUNK = 2048
LANES = 128


def mm(a, b):
    return lax.dot_general(a, b, (((1,), (0,)), ((), ())), preferred_element_type=F32)


def mm_rt(a, b):
    return lax.dot_general(a, b, (((1,), (1,)), ((), ())), preferred_element_type=F32)


def mm_lt(a, b):
    return lax.dot_general(a, b, (((0,), (0,)), ((), ())), preferred_element_type=F32)


def silu_parts(a):
    sig = 0.5 * jnp.tanh(0.5 * a) + 0.5
    act = a * sig
    return act, sig + act * (1.0 - sig)


def norm_parts(b):
    center = b - jnp.mean(b, axis=-1, keepdims=True)
    inv = lax.rsqrt(jnp.mean(center * center, axis=-1, keepdims=True) + EPS)
    return center * inv, inv


def norm_back(g, nrm, inv):
    return inv * (
        g
        - jnp.mean(g, axis=-1, keepdims=True)
        - nrm * jnp.mean(g * nrm, axis=-1, keepdims=True)
    )


def one_hot_cols(low, high, size):
    lane = lax.broadcasted_iota(jnp.int32, low.shape, 1).astype(F32).astype(BF)
    one, zero = jnp.ones_like(low), jnp.zeros_like(low)
    base = jnp.where(low == lane, one, zero)
    tiles = [jnp.where(high == jnp.full_like(high, t), base, zero) for t in range(size // LANES)]
    return jnp.concatenate(tiles, axis=1)


def one_hot_rows(row, size):
    sub = lax.broadcasted_iota(jnp.int32, (size, row.shape[1]), 0)
    return jnp.where(row == sub, 1.0, 0.0).astype(BF)


def my_place():
    j = lax.axis_index("morton")
    return (j >= lax.axis_size("morton") // 2).astype(jnp.int32), j % 2


def spread(row_refs, tmat, outs):
    tmat[...] = jnp.zeros_like(tmat)
    at = 0
    for ref in row_refs:
        for r in range(ref.shape[1] // LANES):
            tmat[at : at + 1, :] = ref[:, r * LANES : (r + 1) * LANES]
            at += 1
    turned = jnp.transpose(tmat[...])
    low = (turned % LANES).astype(F32).astype(BF)
    high = (turned // LANES).astype(F32).astype(BF)
    at = 0
    for ref, (low_ref, high_ref) in zip(row_refs, outs):
        for r in range(ref.shape[1] // LANES):
            rows = slice(r * LANES, (r + 1) * LANES)
            low_ref[rows, :] = jnp.broadcast_to(low[:, at : at + 1], (LANES, LANES))
            high_ref[rows, :] = jnp.broadcast_to(high[:, at : at + 1], (LANES, LANES))
            at += 1


def pack_kernel(meta_ref, h_s, far_ref, one_ref, two_ref, tmat, low, high, got):
    spread([meta_ref.at[:, : low.shape[0]]], tmat, [(low, high)])
    hot = one_hot_cols(low[...], high[...], h_s.shape[0])
    got[...] = mm(hot, h_s[...])
    upper, odd = my_place()
    q = far_ref.shape[0]
    far_ref[...] = got[pl.ds(pl.multiple_of((1 - upper) * 3 * q, q), q), :].astype(BF)
    one_ref[...] = got[pl.ds(pl.multiple_of((2 - odd) * q, q), q), :].astype(BF)
    two_ref[...] = got[pl.ds(pl.multiple_of((1 + odd) * q, q), q), :].astype(BF)


def pre_kernel(
    h_s, e_s, snd_s, rcv_s, w1_s, part_ref, ps_ref, pr_ref, tmat, low_s, high_s, low_r, high_r, rhs
):
    C, H = h_s.shape
    E = e_s.shape[0]
    T = ps_ref.shape[1]
    spread([snd_s, rcv_s], tmat, [(low_s, high_s), (low_r, high_r)])
    w1 = w1_s[...].astype(BF)
    h = h_s[...]
    rhs[0:H, :] = w1[:H]
    rhs[H : H + C, :] = mm(h, w1[H : 2 * H]).astype(BF)
    rhs[H + C :, :] = mm(h, w1[2 * H :]).astype(BF)

    for i in range(E // PRE_CHUNK):
        at = pl.ds(i * PRE_CHUNK, PRE_CHUNK)
        p_s = one_hot_cols(low_s[at, :], high_s[at, :], T)
        p_r = one_hot_cols(low_r[at, :], high_r[at, :], C)
        ps_ref[at, :] = p_s
        pr_ref[at, :] = p_r
        part_ref[at, :] = mm(jnp.concatenate([e_s[at, :], p_s[:, :C], p_r], axis=1), rhs[...])


def main_kernel(
    count_ref, part_ref, ps_ref, pr_ref, far_ref, one_ref, two_ref,
    h_s, e_s, cn_s, ce_s, w1_s, w2_s, eg_s, nw1_s, nw2_s, ng_s,
    gnode_ref, gedge_hbm, bfar_ref, bone_ref, btwo_ref, wmine_ref, woth_ref,
    gh_s, p_s, dsil_s, nrm_s, inv_s, agg, dagg_s, db_s, da_s, gedge_s, wg, dgh, out_sems,
):
    C, H = h_s.shape
    E = e_s.shape[0]
    G = gh_s.shape[0]
    q = G // 4
    upper, odd = my_place()
    gh_s[0:q, :] = far_ref[...]
    gh_s[3 * q :, :] = far_ref[...]
    gh_s[pl.ds(pl.multiple_of((1 + odd) * q, q), q), :] = one_ref[...]
    gh_s[pl.ds(pl.multiple_of((2 - odd) * q, q), q), :] = two_ref[...]
    w1 = w1_s[...].astype(BF)
    w1e, w1s, w1r = w1[:H], w1[H : 2 * H], w1[2 * H :]
    w2 = w2_s[...].astype(BF)
    egain = eg_s[...]
    gtab = mm(gh_s[...], w1s).astype(BF)
    agg[...] = jnp.zeros_like(agg)
    count = count_ref[...]

    def fwd(i, carry):
        at = pl.ds(pl.multiple_of(i * FWD_CHUNK, FWD_CHUNK), FWD_CHUNK)
        act, dsil = silu_parts(part_ref[at, :] + mm(ps_ref[at, C:], gtab))
        p = act.astype(BF)
        p_s[at, :] = p
        dsil_s[at, :] = dsil
        nrm, inv = norm_parts(mm(p, w2))
        nrm_s[at, :] = nrm
        inv_s[at, :] = inv
        rowid = lax.broadcasted_iota(jnp.int32, (FWD_CHUNK, H), 0) + i * FWD_CHUNK
        msg = jnp.where(rowid < count, e_s[at, :].astype(F32) + nrm * egain, 0.0).astype(BF)
        agg[...] += mm_lt(msg, pr_ref[at, :])
        return carry

    lax.fori_loop(0, E // FWD_CHUNK, fwd, 0)

    h = h_s[...]
    nw1 = nw1_s[...].astype(BF)
    nw2 = nw2_s[...].astype(BF)
    cn = cn_s[...].astype(F32)
    aggb = jnp.transpose(agg[...]).astype(BF)
    y = jnp.concatenate([h, aggb], axis=1)
    act, dsil = silu_parts(mm(y, nw1))
    r = act.astype(BF)
    nrm, inv = norm_parts(mm(r, nw2))
    ds = norm_back(cn * ng_s[...], nrm, inv).astype(BF)
    dc = (mm_rt(ds, nw2) * dsil).astype(BF)
    dy = mm_rt(dc, nw1)
    dagg_s[...] = dy[:, H:].astype(BF)
    gnode_ref[...] = cn + dy[:, :H]
    wg[4 * H : 6 * H, :] = mm_lt(y, dc)
    wg[6 * H : 7 * H, :] = mm_lt(r, ds)
    wg[7 * H :, :] = jnp.zeros((wg.shape[0] - 7 * H, H), F32)
    wg[7 * H + 8 : 7 * H + 9, :] = jnp.sum(cn * nrm, axis=0, keepdims=True)

    def out_copy(i):
        at = pl.ds(pl.multiple_of(i * BWD_CHUNK, BWD_CHUNK), BWD_CHUNK)
        return pltpu.make_async_copy(gedge_s.at[at, :], gedge_hbm.at[at, :], out_sems.at[i])

    gain_sum = jnp.zeros((8, H), F32)
    for i in range(E // BWD_CHUNK):
        at = pl.ds(i * BWD_CHUNK, BWD_CHUNK)
        dmsg = mm(pr_ref[at, :], dagg_s[...])
        rowid = lax.broadcasted_iota(jnp.int32, (BWD_CHUNK, H), 0) + i * BWD_CHUNK
        alive = rowid < count
        ce = ce_s[at, :].astype(F32)
        full = ce + dmsg
        d = jnp.where(alive, full, 0.0)
        nrm = nrm_s[at, :]
        gain_sum = gain_sum + jnp.sum((d * nrm).reshape(BWD_CHUNK // 8, 8, H), axis=0)
        db = norm_back(d * egain, nrm, inv_s[at, :]).astype(BF)
        db_s[at, :] = db
        da = (mm_rt(db, w2) * dsil_s[at, :]).astype(BF)
        da_s[at, :] = da
        gedge_s[at, :] = jnp.where(alive, full, ce) + mm_rt(da, w1e)
        out_copy(i).start()

    wg[7 * H : 7 * H + 1, :] = jnp.sum(gain_sum, axis=0, keepdims=True)
    da = da_s[...]
    gs_t = mm_lt(da, ps_ref[...]).astype(BF)
    gr_t = mm_lt(da, pr_ref[...]).astype(BF)
    table = jnp.concatenate([h, gh_s[...]], axis=0)
    wg[3 * H : 4 * H, :] = mm_lt(p_s[...], db_s[...])
    wg[0:H, :] = jnp.transpose(mm_lt(da, e_s[...]))
    wg[H : 2 * H, :] = jnp.transpose(mm(gs_t, table))
    wg[2 * H : 3 * H, :] = jnp.transpose(mm(gr_t, h))
    dt = jnp.transpose(mm(w1s, gs_t))
    gnode_ref[...] += dt[:C] + jnp.transpose(mm(w1r, gr_t))
    dgh[...] = dt[C:]
    bfar_ref[...] = dgh[pl.ds(pl.multiple_of(upper * 3 * q, q), q), :].astype(BF)
    bone_ref[...] = dgh[pl.ds(pl.multiple_of((1 + odd) * q, q), q), :].astype(BF)
    btwo_ref[...] = dgh[pl.ds(pl.multiple_of((2 - odd) * q, q), q), :].astype(BF)
    core = lax.axis_index("dp")
    part = wmine_ref.shape[0]
    wmine_ref[...] = wg[pl.ds(pl.multiple_of(core * part, 8), part), :].astype(BF)
    woth_ref[...] = wg[pl.ds(pl.multiple_of((1 - core) * part, 8), part), :].astype(BF)
    for i in range(E // BWD_CHUNK):
        out_copy(i).wait()


def node_kernel(meta_ref, gnode_ref, far_ref, one_ref, two_ref, out_ref, ret):
    upper, odd = my_place()
    q = far_ref.shape[0]
    ret[...] = jnp.zeros_like(ret)
    ret[pl.ds(pl.multiple_of((1 - upper) * 3 * q, q), q), :] = far_ref[...]
    ret[pl.ds(pl.multiple_of((2 - odd) * q, q), q), :] = one_ref[...]
    ret[pl.ds(pl.multiple_of((1 + odd) * q, q), q), :] = two_ref[...]
    out_ref[...] = gnode_ref[...] + mm(one_hot_rows(meta_ref[:, : ret.shape[0]], out_ref.shape[0]), ret[...])


def unpack_kernel(factor, mine_ref, oth_ref, g1, g2, gg, gn1, gn2, gng, wg):
    core = lax.axis_index("dp")
    part, H = mine_ref.shape
    wg[pl.ds(pl.multiple_of(core * part, 8), part), :] = mine_ref[...].astype(F32) * factor
    wg[pl.ds(pl.multiple_of((1 - core) * part, 8), part), :] = oth_ref[...].astype(F32) * factor
    g1[...] = wg[0 : 3 * H, :]
    g2[...] = wg[3 * H : 4 * H, :]
    gn1[...] = wg[4 * H : 6 * H, :]
    gn2[...] = wg[6 * H : 7 * H, :]
    gg[...] = wg[7 * H : 7 * H + 1, :]
    gng[...] = wg[7 * H + 8 : 7 * H + 9, :]


HBM = pl.BlockSpec(memory_space=pltpu.HBM)
VM = pl.BlockSpec(memory_space=pltpu.VMEM)
MIB = 1024 * 1024


def sds(shape, dtype):
    return jax.ShapeDtypeStruct(shape, dtype)


def call(kernel, outs, in_specs, out_specs, scratch, flops, nbytes, limit):
    return pl.pallas_call(
        kernel,
        out_shape=outs,
        in_specs=in_specs,
        out_specs=out_specs,
        scratch_shapes=scratch,
        compiler_params=pltpu.CompilerParams(vmem_limit_bytes=limit * MIB),
        cost_estimate=pl.CostEstimate(flops=flops, bytes_accessed=nbytes, transcendentals=0),
    )


def flip(x, axis, by):
    n = lax.axis_size(axis)
    return lax.ppermute(x, axis, [(i, i ^ by) for i in range(n)])


def cross_pairs(x):
    n = lax.axis_size("morton")
    pairs = [(i, (i + 1 if i % 2 else i - 1) % n) for i in range(n)]
    return lax.ppermute(x, "morton", pairs)


def pick(x, k):
    return lax.dynamic_index_in_dim(x, k, 0, keepdims=False)


def tree_sum(parts):
    while len(parts) > 1:
        parts = [parts[i] + parts[i + 1] for i in range(0, len(parts), 2)]
    return parts[0]


def stages_of(n):
    out = []
    stride = 1
    while stride < n:
        w = 4 if n // stride >= 4 else 2
        out.append((stride, w))
        stride *= w
    return out


def flip_with(x, by, extra, got):
    if by in extra:
        rider = extra.pop(by)
        moved = flip(jnp.concatenate([x, rider], axis=0), "morton", by)
        got[by] = moved[x.shape[0] :]
        return moved[: x.shape[0]]
    return flip(x, "morton", by)


def reduce_all(mine, oth, extra, early, finish):
    got = {}
    stages = stages_of(lax.axis_size("morton"))
    v = mine.astype(F32) + flip(oth, "dp", 1).astype(F32)
    low = lax.axis_index("morton") % 2
    halves = v.astype(BF).reshape(2, v.shape[0] // 2, v.shape[1])
    kept, given = pick(halves, low), pick(halves, 1 - low)
    parts = [kept.astype(F32)]
    for d in range(1, stages[0][1]):
        moved = flip_with(given if d % 2 else kept, d, extra, got)
        parts.append(moved.astype(F32))
    v, early = lax.optimization_barrier((tree_sum(parts), early))
    for stride, width in stages[1:]:
        w = v.astype(BF)
        parts = [w.astype(F32)]
        for d in range(1, width):
            parts.append(flip_with(w, d * stride, extra, got).astype(F32))
        v = tree_sum(parts)
    for by in list(extra):
        got[by] = flip(extra.pop(by), "morton", by)
    w = v.astype(BF)
    back = flip(w, "morton", 1)
    both = jnp.stack([w, back])
    mine = jnp.concatenate([pick(both, low), pick(both, 1 - low)], axis=0)
    mine, done = lax.optimization_barrier((mine, finish(early, got)))
    return mine, flip(mine, "dp", 1), done


def local_step(
    node_feat, edge_feat, cot_node, cot_edge, senders, receivers, send_rows, edge_count,
    edge_w1, edge_w2, edge_gain, node_w1, node_w2, node_gain,
):
    peers = lax.axis_size("morton")
    pair = lax.axis_size("dp")
    half = peers // 2
    h, e, cn, ce = node_feat[0], edge_feat[0], cot_node[0], cot_edge[0]
    C, H = h.shape
    E = e.shape[0]
    G = send_rows.shape[1]
    q = G // 4
    T = C + G
    i32 = jnp.int32
    meta = jnp.maximum(send_rows, 0)
    dma = pltpu.SemaphoreType.DMA
    egain, ngain = edge_gain.reshape(1, H), node_gain.reshape(1, H)

    ghost = sds((q, H), BF)
    far, one, two = call(
        pack_kernel, (ghost,) * 3, [VM] * 2, (VM,) * 3,
        [pltpu.VMEM((LANES, LANES), i32), pltpu.VMEM((G, LANES), BF),
         pltpu.VMEM((G, LANES), BF), pltpu.VMEM((G, H), F32)],
        4_000_000_000, 8_000_000, 8,
    )(meta, h)
    far = flip(far, "morton", half)
    one = flip(one, "morton", 1)
    two = cross_pairs(two)

    part, ps, pr = call(
        pre_kernel, (sds((E, H), F32), sds((E, T), BF), sds((E, C), BF)),
        [VM] * 5, (VM,) * 3,
        [pltpu.VMEM((LANES, LANES), i32)] + [pltpu.VMEM((E, LANES), BF)] * 4
        + [pltpu.VMEM((H + 2 * C, H), BF)],
        2 * E * H * (H + 2 * C) * 4, 4 * E * (H + T), 24,
    )(h, e, senders, receivers, edge_w1)

    rows = -(-(7 * H + 16) // (pair * 16)) * (pair * 16)
    mine_shape = sds((rows // pair, H), BF)
    layer_in = [h, e, cn, ce, edge_w1, edge_w2, egain, node_w1, node_w2, ngain]
    gnode, gedge, bfar, bone, btwo, wmine, woth = call(
        main_kernel,
        (sds((C, H), F32), sds((E, H), F32), ghost, ghost, ghost, mine_shape, mine_shape),
        [VM] * 17,
        (VM, HBM, VM, VM, VM, VM, VM),
        [pltpu.VMEM((G, H), BF), pltpu.VMEM((E, H), BF), pltpu.VMEM((E, H), F32),
           pltpu.VMEM((E, H), F32), pltpu.VMEM((E, 1), F32), pltpu.VMEM((H, C), F32),
           pltpu.VMEM((C, H), BF), pltpu.VMEM((E, H), BF), pltpu.VMEM((E, H), BF),
           pltpu.VMEM((E, H), F32), pltpu.VMEM((rows, H), F32), pltpu.VMEM((G, H), F32),
           dma((E // BWD_CHUNK,))],
        2 * E * H * 4608, 8 * E * H, 36,
    )(edge_count, part, ps, pr, far, one, two, *layer_in)

    def finish(rtwo, got):
        return call(
            node_kernel, sds((C, H), F32), [VM] * 5, VM,
            [pltpu.VMEM((G, H), BF)],
            2 * C * G * H, 8 * C * H, 8,
        )(meta, gnode, got[half], got[1], rtwo)

    rtwo = cross_pairs(btwo)
    mine, oth, grad_node = reduce_all(wmine, woth, {1: bone, half: bfar}, rtwo, finish)
    factor = float(pair * peers * E) ** -0.5
    g1, g2, gg, gn1, gn2, gng = call(
        functools.partial(unpack_kernel, factor),
        tuple(sds(s, F32) for s in ((3 * H, H), (H, H), (1, H), (2 * H, H), (H, H), (1, H))),
        [VM] * 2, (VM,) * 6, [pltpu.VMEM((rows, H), F32)], rows * H, 8 * rows * H, 8,
    )(mine, oth)
    return (
        grad_node[None], gedge[None], g1, g2, gg.reshape(H), gn1, gn2, gng.reshape(H),
    )


def solution(mesh):
    cells = P("dp", "morton", None)
    flat = P("dp", "morton")
    in_specs = (cells,) * 4 + (flat,) * 4 + (P(),) * 6
    out_specs = (cells, cells) + (P(),) * 6
    return jax.shard_map(
        local_step, mesh=mesh, in_specs=in_specs, out_specs=out_specs, check_vma=False
    )
```

```python
import functools

import jax
import jax.numpy as jnp
from jax import lax
from jax.experimental import pallas as pl
from jax.experimental.pallas import tpu as pltpu
from jax.sharding import PartitionSpec as P


BF = jnp.bfloat16
F32 = jnp.float32
EPS = 1e-05
PRE_CHUNK = 1024
FWD_CHUNK = 2048
BWD_CHUNK = 2048
LANES = 128


def mm(a, b):
    return lax.dot_general(a, b, (((1,), (0,)), ((), ())), preferred_element_type=F32)


def mm_rt(a, b):
    return lax.dot_general(a, b, (((1,), (1,)), ((), ())), preferred_element_type=F32)


def mm_lt(a, b):
    return lax.dot_general(a, b, (((0,), (0,)), ((), ())), preferred_element_type=F32)


def silu_parts(a):
    sig = 0.5 * jnp.tanh(0.5 * a) + 0.5
    act = a * sig
    return act, sig + act * (1.0 - sig)


def norm_parts(b):
    center = b - jnp.mean(b, axis=-1, keepdims=True)
    inv = lax.rsqrt(jnp.mean(center * center, axis=-1, keepdims=True) + EPS)
    return center * inv, inv


def norm_back(g, nrm, inv):
    return inv * (
        g
        - jnp.mean(g, axis=-1, keepdims=True)
        - nrm * jnp.mean(g * nrm, axis=-1, keepdims=True)
    )


def one_hot_cols(low, high, size):
    lane = lax.broadcasted_iota(jnp.int32, low.shape, 1).astype(F32).astype(BF)
    one, zero = jnp.ones_like(low), jnp.zeros_like(low)
    base = jnp.where(low == lane, one, zero)
    tiles = [jnp.where(high == jnp.full_like(high, t), base, zero) for t in range(size // LANES)]
    return jnp.concatenate(tiles, axis=1)


def one_hot_rows(row, size):
    sub = lax.broadcasted_iota(jnp.int32, (size, row.shape[1]), 0)
    return jnp.where(row == sub, 1.0, 0.0).astype(BF)


def my_place():
    j = lax.axis_index("morton")
    return (j >= lax.axis_size("morton") // 2).astype(jnp.int32), j % 2


def spread(row_refs, tmat, outs):
    tmat[...] = jnp.zeros_like(tmat)
    at = 0
    for ref in row_refs:
        for r in range(ref.shape[1] // LANES):
            tmat[at : at + 1, :] = ref[:, r * LANES : (r + 1) * LANES]
            at += 1
    turned = jnp.transpose(tmat[...])
    low = (turned % LANES).astype(F32).astype(BF)
    high = (turned // LANES).astype(F32).astype(BF)
    at = 0
    for ref, (low_ref, high_ref) in zip(row_refs, outs):
        for r in range(ref.shape[1] // LANES):
            rows = slice(r * LANES, (r + 1) * LANES)
            low_ref[rows, :] = jnp.broadcast_to(low[:, at : at + 1], (LANES, LANES))
            high_ref[rows, :] = jnp.broadcast_to(high[:, at : at + 1], (LANES, LANES))
            at += 1


def digits_kernel(meta_ref, low, high, tmat):
    spread([meta_ref], tmat, [(low, high)])


def pack_kernel(low, high, h_s, far_ref, one_ref, two_ref, got):
    hot = one_hot_cols(low[...], high[...], h_s.shape[0])
    got[...] = mm(hot, h_s[...])
    upper, odd = my_place()
    q = far_ref.shape[0]
    far_ref[...] = got[pl.ds(pl.multiple_of((1 - upper) * 3 * q, q), q), :].astype(BF)
    one_ref[...] = got[pl.ds(pl.multiple_of((2 - odd) * q, q), q), :].astype(BF)
    two_ref[...] = got[pl.ds(pl.multiple_of((1 + odd) * q, q), q), :].astype(BF)


def pre_kernel(
    h_s, e_s, snd_s, rcv_s, w1_s, part_ref, ps_ref, pr_ref, tmat, low_s, high_s, low_r, high_r, rhs
):
    C, H = h_s.shape
    E = e_s.shape[0]
    T = ps_ref.shape[1]
    spread([snd_s, rcv_s], tmat, [(low_s, high_s), (low_r, high_r)])
    w1 = w1_s[...].astype(BF)
    h = h_s[...]
    rhs[0:H, :] = w1[:H]
    rhs[H : H + C, :] = mm(h, w1[H : 2 * H]).astype(BF)
    rhs[H + C :, :] = mm(h, w1[2 * H :]).astype(BF)

    for i in range(E // PRE_CHUNK):
        at = pl.ds(i * PRE_CHUNK, PRE_CHUNK)
        p_s = one_hot_cols(low_s[at, :], high_s[at, :], T)
        p_r = one_hot_cols(low_r[at, :], high_r[at, :], C)
        ps_ref[at, :] = p_s
        pr_ref[at, :] = p_r
        part_ref[at, :] = mm(jnp.concatenate([e_s[at, :], p_s[:, :C], p_r], axis=1), rhs[...])


def main_kernel(
    count_ref, part_ref, ps_ref, pr_ref, far_ref, one_ref, two_ref,
    h_s, e_s, cn_s, ce_s, w1_s, w2_s, eg_s, nw1_s, nw2_s, ng_s,
    gnode_ref, gedge_hbm, bfar_ref, bone_ref, btwo_ref, wmine_ref, woth_ref,
    gh_s, p_s, dsil_s, nrm_s, inv_s, agg, dagg_s, db_s, da_s, gedge_s, wg, dgh, out_sems,
):
    C, H = h_s.shape
    E = e_s.shape[0]
    G = gh_s.shape[0]
    q = G // 4
    upper, odd = my_place()
    gh_s[0:q, :] = far_ref[...]
    gh_s[3 * q :, :] = far_ref[...]
    gh_s[pl.ds(pl.multiple_of((1 + odd) * q, q), q), :] = one_ref[...]
    gh_s[pl.ds(pl.multiple_of((2 - odd) * q, q), q), :] = two_ref[...]
    w1 = w1_s[...].astype(BF)
    w1e, w1s, w1r = w1[:H], w1[H : 2 * H], w1[2 * H :]
    w2 = w2_s[...].astype(BF)
    egain = eg_s[...]
    gtab = mm(gh_s[...], w1s).astype(BF)
    agg[...] = jnp.zeros_like(agg)
    count = count_ref[...]

    def fwd(i, carry):
        at = pl.ds(pl.multiple_of(i * FWD_CHUNK, FWD_CHUNK), FWD_CHUNK)
        act, dsil = silu_parts(part_ref[at, :] + mm(ps_ref[at, C:], gtab))
        p = act.astype(BF)
        p_s[at, :] = p
        dsil_s[at, :] = dsil
        nrm, inv = norm_parts(mm(p, w2))
        nrm_s[at, :] = nrm
        inv_s[at, :] = inv
        rowid = lax.broadcasted_iota(jnp.int32, (FWD_CHUNK, H), 0) + i * FWD_CHUNK
        msg = jnp.where(rowid < count, e_s[at, :].astype(F32) + nrm * egain, 0.0).astype(BF)
        agg[...] += mm_lt(msg, pr_ref[at, :])
        return carry

    lax.fori_loop(0, E // FWD_CHUNK, fwd, 0)

    h = h_s[...]
    nw1 = nw1_s[...].astype(BF)
    nw2 = nw2_s[...].astype(BF)
    cn = cn_s[...].astype(F32)
    aggb = jnp.transpose(agg[...]).astype(BF)
    y = jnp.concatenate([h, aggb], axis=1)
    act, dsil = silu_parts(mm(y, nw1))
    r = act.astype(BF)
    nrm, inv = norm_parts(mm(r, nw2))
    ds = norm_back(cn * ng_s[...], nrm, inv).astype(BF)
    dc = (mm_rt(ds, nw2) * dsil).astype(BF)
    dy = mm_rt(dc, nw1)
    dagg_s[...] = dy[:, H:].astype(BF)
    gnode_ref[...] = cn + dy[:, :H]
    wg[4 * H : 6 * H, :] = mm_lt(y, dc)
    wg[6 * H : 7 * H, :] = mm_lt(r, ds)
    wg[7 * H :, :] = jnp.zeros((wg.shape[0] - 7 * H, H), F32)
    wg[7 * H + 8 : 7 * H + 9, :] = jnp.sum(cn * nrm, axis=0, keepdims=True)

    def out_copy(i):
        at = pl.ds(pl.multiple_of(i * BWD_CHUNK, BWD_CHUNK), BWD_CHUNK)
        return pltpu.make_async_copy(gedge_s.at[at, :], gedge_hbm.at[at, :], out_sems.at[i])

    gain_sum = jnp.zeros((8, H), F32)
    for i in range(E // BWD_CHUNK):
        at = pl.ds(i * BWD_CHUNK, BWD_CHUNK)
        dmsg = mm(pr_ref[at, :], dagg_s[...])
        rowid = lax.broadcasted_iota(jnp.int32, (BWD_CHUNK, H), 0) + i * BWD_CHUNK
        alive = rowid < count
        ce = ce_s[at, :].astype(F32)
        full = ce + dmsg
        d = jnp.where(alive, full, 0.0)
        nrm = nrm_s[at, :]
        gain_sum = gain_sum + jnp.sum((d * nrm).reshape(BWD_CHUNK // 8, 8, H), axis=0)
        db = norm_back(d * egain, nrm, inv_s[at, :]).astype(BF)
        db_s[at, :] = db
        da = (mm_rt(db, w2) * dsil_s[at, :]).astype(BF)
        da_s[at, :] = da
        gedge_s[at, :] = jnp.where(alive, full, ce) + mm_rt(da, w1e)
        out_copy(i).start()

    wg[7 * H : 7 * H + 1, :] = jnp.sum(gain_sum, axis=0, keepdims=True)
    da = da_s[...]
    gs_t = mm_lt(da, ps_ref[...]).astype(BF)
    gr_t = mm_lt(da, pr_ref[...]).astype(BF)
    table = jnp.concatenate([h, gh_s[...]], axis=0)
    wg[3 * H : 4 * H, :] = mm_lt(p_s[...], db_s[...])
    wg[0:H, :] = jnp.transpose(mm_lt(da, e_s[...]))
    wg[H : 2 * H, :] = jnp.transpose(mm(gs_t, table))
    wg[2 * H : 3 * H, :] = jnp.transpose(mm(gr_t, h))
    dt = jnp.transpose(mm(w1s, gs_t))
    gnode_ref[...] += dt[:C] + jnp.transpose(mm(w1r, gr_t))
    dgh[...] = dt[C:]
    bfar_ref[...] = dgh[pl.ds(pl.multiple_of(upper * 3 * q, q), q), :].astype(BF)
    bone_ref[...] = dgh[pl.ds(pl.multiple_of((1 + odd) * q, q), q), :].astype(BF)
    btwo_ref[...] = dgh[pl.ds(pl.multiple_of((2 - odd) * q, q), q), :].astype(BF)
    core = lax.axis_index("dp")
    part = wmine_ref.shape[0]
    wmine_ref[...] = wg[pl.ds(pl.multiple_of(core * part, 8), part), :].astype(BF)
    woth_ref[...] = wg[pl.ds(pl.multiple_of((1 - core) * part, 8), part), :].astype(BF)
    for i in range(E // BWD_CHUNK):
        out_copy(i).wait()


def node_kernel(meta_ref, gnode_ref, far_ref, one_ref, two_ref, out_ref, ret):
    upper, odd = my_place()
    q = far_ref.shape[0]
    ret[...] = jnp.zeros_like(ret)
    ret[pl.ds(pl.multiple_of((1 - upper) * 3 * q, q), q), :] = far_ref[...]
    ret[pl.ds(pl.multiple_of((2 - odd) * q, q), q), :] = one_ref[...]
    ret[pl.ds(pl.multiple_of((1 + odd) * q, q), q), :] = two_ref[...]
    out_ref[...] = gnode_ref[...] + mm(one_hot_rows(meta_ref[:, : ret.shape[0]], out_ref.shape[0]), ret[...])


def unpack_kernel(factor, p0, p1, p2, p3, g1, g2, gg, gn1, gn2, gng, wg):
    core = lax.axis_index("dp")
    low = lax.axis_index("morton") % 2
    part, H = p0.shape
    for ref, by, core_by in ((p0, 0, 0), (p1, 1, 0), (p2, 0, 1), (p3, 1, 1)):
        side = core if core_by == 0 else 1 - core
        bit = low if by == 0 else 1 - low
        at = pl.multiple_of((2 * side + bit) * part, 8)
        wg[pl.ds(at, part), :] = ref[...].astype(F32) * factor
    g1[...] = wg[0 : 3 * H, :]
    g2[...] = wg[3 * H : 4 * H, :]
    gn1[...] = wg[4 * H : 6 * H, :]
    gn2[...] = wg[6 * H : 7 * H, :]
    gg[...] = wg[7 * H : 7 * H + 1, :]
    gng[...] = wg[7 * H + 8 : 7 * H + 9, :]


HBM = pl.BlockSpec(memory_space=pltpu.HBM)
VM = pl.BlockSpec(memory_space=pltpu.VMEM)
MIB = 1024 * 1024


def sds(shape, dtype):
    return jax.ShapeDtypeStruct(shape, dtype)


def call(kernel, outs, in_specs, out_specs, scratch, flops, nbytes, limit):
    return pl.pallas_call(
        kernel,
        out_shape=outs,
        in_specs=in_specs,
        out_specs=out_specs,
        scratch_shapes=scratch,
        compiler_params=pltpu.CompilerParams(vmem_limit_bytes=limit * MIB),
        cost_estimate=pl.CostEstimate(flops=flops, bytes_accessed=nbytes, transcendentals=0),
    )


def flip(x, axis, by):
    n = lax.axis_size(axis)
    return lax.ppermute(x, axis, [(i, i ^ by) for i in range(n)])


def flip_both(x, by, core_by):
    n, pair = lax.axis_size("morton"), lax.axis_size("dp")
    moves = [
        (m * pair + d, (m ^ by) * pair + (d ^ core_by)) for m in range(n) for d in range(pair)
    ]
    return lax.ppermute(x, ("morton", "dp"), moves)


def cross_pairs(x):
    n = lax.axis_size("morton")
    pairs = [(i, (i + 1 if i % 2 else i - 1) % n) for i in range(n)]
    return lax.ppermute(x, "morton", pairs)


def pick(x, k):
    return lax.dynamic_index_in_dim(x, k, 0, keepdims=False)


def tree_sum(parts):
    while len(parts) > 1:
        parts = [parts[i] + parts[i + 1] for i in range(0, len(parts), 2)]
    return parts[0]


def stages_of(n):
    out = []
    stride = 1
    while stride < n:
        w = 4 if n // stride >= 4 else 2
        out.append((stride, w))
        stride *= w
    return out


def flip_with(x, by, extra, got):
    if by in extra:
        rider = extra.pop(by)
        moved = flip(jnp.concatenate([x, rider], axis=0), "morton", by)
        got[by] = moved[x.shape[0] :]
        return moved[: x.shape[0]]
    return flip(x, "morton", by)


def reduce_all(mine, oth, extra, early, finish):
    got = {}
    stages = stages_of(lax.axis_size("morton"))
    v = mine.astype(F32) + flip(oth, "dp", 1).astype(F32)
    low = lax.axis_index("morton") % 2
    halves = v.astype(BF).reshape(2, v.shape[0] // 2, v.shape[1])
    kept, given = pick(halves, low), pick(halves, 1 - low)
    parts = [kept.astype(F32)]
    for d in range(1, stages[0][1]):
        moved = flip_with(given if d % 2 else kept, d, extra, got)
        parts.append(moved.astype(F32))
    v, early = lax.optimization_barrier((tree_sum(parts), early))
    for stride, width in stages[1:]:
        w = v.astype(BF)
        parts = [w.astype(F32)]
        for d in range(1, width):
            parts.append(flip_with(w, d * stride, extra, got).astype(F32))
        v = tree_sum(parts)
    for by in list(extra):
        got[by] = flip(extra.pop(by), "morton", by)
    w = v.astype(BF)
    parts = [w, flip_both(w, 1, 0), flip_both(w, 0, 1), flip_both(w, 1, 1)]
    return parts, finish(early, got)


def local_step(
    node_feat, edge_feat, cot_node, cot_edge, senders, receivers, send_rows, edge_count,
    edge_w1, edge_w2, edge_gain, node_w1, node_w2, node_gain,
):
    peers = lax.axis_size("morton")
    pair = lax.axis_size("dp")
    half = peers // 2
    h, e, cn, ce = node_feat[0], edge_feat[0], cot_node[0], cot_edge[0]
    C, H = h.shape
    E = e.shape[0]
    G = send_rows.shape[1]
    q = G // 4
    T = C + G
    i32 = jnp.int32
    dma = pltpu.SemaphoreType.DMA
    egain, ngain = edge_gain.reshape(1, H), node_gain.reshape(1, H)

    ghost = sds((q, H), BF)
    low, high = call(
        digits_kernel, (sds((G, LANES), BF),) * 2, [VM], (VM,) * 2,
        [pltpu.VMEM((LANES, LANES), i32)], 4_000_000_000, 8_000_000, 8,
    )(send_rows)
    far, one, two = call(
        pack_kernel, (ghost,) * 3, [VM] * 3, (VM,) * 3,
        [pltpu.VMEM((G, H), F32)], 4_000_000_000, 8_000_000, 8,
    )(low, high, h)
    far = flip(far, "morton", half)
    one = flip(one, "morton", 1)
    two = cross_pairs(two)

    part, ps, pr = call(
        pre_kernel, (sds((E, H), F32), sds((E, T), BF), sds((E, C), BF)),
        [VM] * 5, (VM,) * 3,
        [pltpu.VMEM((LANES, LANES), i32)] + [pltpu.VMEM((E, LANES), BF)] * 4
        + [pltpu.VMEM((H + 2 * C, H), BF)],
        2 * E * H * (H + 2 * C) * 4, 4 * E * (H + T), 24,
    )(h, e, senders, receivers, edge_w1)

    rows = -(-(7 * H + 16) // (pair * 16)) * (pair * 16)
    mine_shape = sds((rows // pair, H), BF)
    layer_in = [h, e, cn, ce, edge_w1, edge_w2, egain, node_w1, node_w2, ngain]
    gnode, gedge, bfar, bone, btwo, wmine, woth = call(
        main_kernel,
        (sds((C, H), F32), sds((E, H), F32), ghost, ghost, ghost, mine_shape, mine_shape),
        [VM] * 17,
        (VM, HBM, VM, VM, VM, VM, VM),
        [pltpu.VMEM((G, H), BF), pltpu.VMEM((E, H), BF), pltpu.VMEM((E, H), F32),
           pltpu.VMEM((E, H), F32), pltpu.VMEM((E, 1), F32), pltpu.VMEM((H, C), F32),
           pltpu.VMEM((C, H), BF), pltpu.VMEM((E, H), BF), pltpu.VMEM((E, H), BF),
           pltpu.VMEM((E, H), F32), pltpu.VMEM((rows, H), F32), pltpu.VMEM((G, H), F32),
           dma((E // BWD_CHUNK,))],
        2 * E * H * 4608, 8 * E * H, 36,
    )(edge_count, part, ps, pr, far, one, two, *layer_in)

    def finish(rtwo, got):
        return call(
            node_kernel, sds((C, H), F32), [VM] * 5, VM,
            [pltpu.VMEM((G, H), BF)],
            2 * C * G * H, 8 * C * H, 8,
        )(send_rows, gnode, got[half], got[1], rtwo)

    rtwo = cross_pairs(btwo)
    pieces, grad_node = reduce_all(wmine, woth, {1: bone, half: bfar}, rtwo, finish)
    factor = float(pair * peers * E) ** -0.5
    g1, g2, gg, gn1, gn2, gng = call(
        functools.partial(unpack_kernel, factor),
        tuple(sds(s, F32) for s in ((3 * H, H), (H, H), (1, H), (2 * H, H), (H, H), (1, H))),
        [VM] * 4, (VM,) * 6, [pltpu.VMEM((rows, H), F32)], rows * H, 8 * rows * H, 8,
    )(*pieces)
    return (
        grad_node[None], gedge[None], g1, g2, gg.reshape(H), gn1, gn2, gng.reshape(H),
    )


def solution(mesh):
    cells = P("dp", "morton", None)
    flat = P("dp", "morton")
    in_specs = (cells,) * 4 + (flat,) * 4 + (P(),) * 6
    out_specs = (cells, cells) + (P(),) * 6
    return jax.shard_map(
        local_step, mesh=mesh, in_specs=in_specs, out_specs=out_specs, check_vma=False
    )
```
